256 devices in a mesh: row: 4 (over x), col: 32 (over y, z), batch: 2 (over core).
Axes of the slice: x: 4, y: 4, z: 8, core: 2. Of those that a mesh axis runs over, the one named last changes fastest.
Arguments:
- item_ids: int32 [4, 32, 2048], P('batch', 'col', 'row'), parts along dimension 0, may hold values from 0 to 511
- pad_masks: int32 [4, 32, 2048], P('batch', 'col', 'row'), parts along dimension 0, may hold values from 0 to 1
- lengths: int32 [4], P('batch'), parts along dimension 0, may hold values from 64512 to 65536
- item_table: bfloat16 [512, 1024], replicated, may hold values from -5 to 5
- w_gate: bfloat16 [1024, 1024], replicated, may hold values from -0.1875 to 0.1875
- w_in: bfloat16 [1024, 1280], replicated, may hold values from -0.1875 to 0.1875
- w_dt: bfloat16 [1024, 8], replicated, may hold values from -0.1875 to 0.1875
- conv_taps: float32 [4, 1280], replicated, may hold values from -3 to 3
- dt_bias: float32 [8], replicated, may hold values from -2 to 1
- decay_rates: float32 [8], replicated, may hold values from 1.5258789e-06 to 0.05
- norm_gain: float32 [1024], replicated, may hold values from 0.1 to 1.9
- w_out: bfloat16 [1024, 1024], replicated, may hold values from -0.1875 to 0.1875
Outputs:
- result: bfloat16 [4, 32, 2048, 1024], P('batch', 'col', 'row'), parts along dimension 0
The draws below stay inside these ranges and needn't reach their ends.
There are 2 independent parts, one for each index of `batch`. The reference program is written for one: setup_inputs(seed, part) draws one part's arguments, and reference() takes and returns one part's arrays. A program takes and returns all parts, laid end to end along the dimension named above; an argument that names none is the same for every part. Nothing has to cross between parts.
Inputs may be any that keep to these rules, and one draw needn't show every extreme that they name: `lengths`: every history keeps at least its first 64512 positions before padding.
All inputs are finite; a program needn't handle non-finite values.
Results may differ from the reference program's by a relative error of at most 0.0093.
Values may be sent and summed in bfloat16 or wider, within the bound.
A program may use at most 128 MiB of HBM per device.

```python
import math
import jax
import jax.numpy as jnp
import numpy as np
from jax import lax

D = 1024
H = 8
NS = 128
KW = 4
STRETCH = 128
ITEMS = 512
SEQS = 2
TOK_DEV = 512
DI = 1024
BLOCKS = 32
BLOCK_LEN = 2048
LENGTH = 65536


def draw_pad_masks(key, part):
    level_key = jax.random.fold_in(key, 17)
    entry_key = jax.random.fold_in(key, 29)
    spans = BLOCK_LEN // TOK_DEV
    levels = jax.random.randint(level_key, (SEQS, BLOCKS, spans, 1), 1, 5, dtype=jnp.int32)
    entries = jax.random.randint(entry_key, (SEQS, BLOCKS, spans, TOK_DEV), 0, 4, dtype=jnp.int32)
    kept = (entries < levels).astype(jnp.int32)
    return kept.reshape(SEQS, BLOCKS, BLOCK_LEN)


def place_ends(values, key, least, largest):
    dims = values.shape
    spot = [jax.random.randint(jax.random.fold_in(key, axis), (), 0, dims[axis]) for axis in range(len(dims))]
    values = values.at[tuple(spot)].set(least)
    longest = dims.index(max(dims))
    spot[longest] = (spot[longest] + 1) % dims[longest]
    return values.at[tuple(spot)].set(largest)


def cumulative_ranks(number_of, skew):
    loads = [(1 << 20) // math.isqrt(grade ** skew) + 1 for grade in range(1, number_of + 1)]
    deviation = 1 + sum(loads) // (1 << 30)
    return np.cumsum(np.array([max(1, weight // deviation) for weight in loads]))


def ranked_ids(rng, shape, count, skew):
    listing = cumulative_ranks(count, skew)
    lot = jax.random.randint(jax.random.fold_in(rng, 1), shape, 0, int(listing[count - 1]))
    rank = jnp.searchsorted(jnp.asarray(listing, jnp.int32), lot, side="right")
    return jax.random.permutation(jax.random.fold_in(rng, 2), count)[rank].astype(jnp.int32)


def gaussian(rng, extent, width, bound, kind=jnp.bfloat16):
    array = jax.random.normal(rng, extent, jnp.float32) * width
    return jnp.minimum(jnp.maximum(array, -bound), bound).astype(kind)


def setup_inputs(seed: int = 0, part: int = 0) -> dict:
    key_list = jax.random.split(jax.random.key(seed), 13)
    part_keys = jax.random.split(jax.random.fold_in(key_list[12], part), 13)
    return {
        "item_ids": place_ends(ranked_ids(part_keys[0], (SEQS, BLOCKS, BLOCK_LEN), ITEMS, 2), jax.random.fold_in(part_keys[0], 3), 0, ITEMS - 1).astype(jnp.int32),
        "pad_masks": draw_pad_masks(jax.random.fold_in(jax.random.fold_in(key_list[12], part), 71), part),
        "lengths": jax.random.randint(part_keys[2], (SEQS,), LENGTH - BLOCK_LEN // 2, LENGTH + 1).astype(jnp.int32),
        "item_table": gaussian(key_list[3], (ITEMS, D), 1.0, 5.0),
        "w_gate": gaussian(key_list[4], (D, DI), D ** -0.5, 0.1875),
        "w_in": gaussian(key_list[5], (D, DI + 2 * NS), D ** -0.5, 0.1875),
        "w_dt": gaussian(key_list[6], (D, H), D ** -0.5, 0.1875),
        "conv_taps": gaussian(key_list[7], (KW, DI + 2 * NS), 0.5, 3.0, jnp.float32),
        "dt_bias": jnp.clip(jax.random.uniform(key_list[8], (H,), jnp.float32, -2.0, 1.0), -2.0, 1.0),
        "decay_rates": jnp.clip(jnp.exp(jax.random.uniform(key_list[9], (H,), jnp.float32, math.log(1.5258789289873675e-06), math.log(0.05))), 1.5258789289873675e-06, 0.05),
        "norm_gain": jnp.clip(1.0 + 0.18 * jax.random.normal(key_list[10], (DI,), jnp.float32), 0.1, 1.9),
        "w_out": gaussian(key_list[11], (DI, D), DI ** -0.5, 0.1875),
    }


def rounded(value):
    return lax.optimization_barrier(value.astype(jnp.bfloat16)).astype(jnp.float32)

def reference(item_ids, pad_masks, lengths, item_table, w_gate, w_in, w_dt, conv_taps, dt_bias, decay_rates, norm_gain, w_out):
    users = item_ids.shape[0]
    events = item_ids.shape[1] * item_ids.shape[2]
    stretch_count = events // STRETCH
    full_width = w_in.shape[1]
    inner_width = w_gate.shape[1]
    head_count = decay_rates.shape[0]
    head_size = inner_width // head_count
    state_width = (full_width - inner_width) // 2
    kernel = conv_taps.shape[0]
    item_stretches = item_ids.reshape(users, stretch_count, STRETCH).transpose(1, 0, 2)
    mask_stretches = pad_masks.reshape(users, stretch_count, STRETCH).transpose(1, 0, 2)
    starts = jnp.arange(stretch_count, dtype=jnp.int32) * STRETCH
    within = jnp.arange(STRETCH, dtype=jnp.int32)
    causal = within[:, None] >= within[None, :]

    def advance(carried, inputs):
        state_now, before = carried
        item_rows, mask_rows, start = inputs
        embedded = jnp.take(item_table, item_rows, axis=0).reshape(users * STRETCH, -1)
        projected = jnp.dot(embedded, w_in, preferred_element_type=jnp.float32).astype(jnp.bfloat16).reshape(users, STRETCH, full_width)
        gate_rows = rounded(jnp.dot(embedded, w_gate, preferred_element_type=jnp.float32)).reshape(users, STRETCH, inner_width)
        step_raw = jnp.dot(embedded, w_dt, preferred_element_type=jnp.float32).reshape(users, STRETCH, head_count)
        joined = lax.optimization_barrier(jnp.concatenate([before, projected], axis=1)).astype(jnp.float32)
        convolved = joined[:, 0:STRETCH, :] * conv_taps[0]
        for offset in range(1, kernel):
            convolved = convolved + joined[:, offset:offset + STRETCH, :] * conv_taps[offset]
        signal = rounded(jax.nn.silu(convolved[..., :inner_width]))
        inward = rounded(convolved[..., inner_width:inner_width + state_width])
        outward = rounded(convolved[..., inner_width + state_width:])
        position = start + within
        usable = jnp.logical_and(position[None, :] < lengths[:, None], mask_rows > 0).astype(jnp.float32)
        step_size = usable[..., None] * jax.nn.softplus(step_raw + dt_bias)
        log_decay = jnp.cumsum(step_size * decay_rates, axis=1)
        log_heads = log_decay.transpose(0, 2, 1)
        size_heads = step_size.transpose(0, 2, 1)
        scores = jnp.einsum('sqn,sun->squ', outward, inward)
        log_gap = log_heads[:, :, :, None] - log_heads[:, :, None, :]
        decays = jnp.where(causal, jnp.exp(-jnp.where(causal, log_gap, 0.0)), 0.0)
        weights = rounded(scores[:, None] * decays * size_heads[:, :, None, :])
        signal_heads = signal.reshape(users, STRETCH, head_count, head_size)
        local_out = jnp.einsum('shqu,suhp->sqhp', weights, signal_heads)
        entering = rounded(state_now)
        carried_out = jnp.einsum('sqn,shpn->sqhp', outward, entering) * jnp.exp(-log_decay)[..., None]
        mixture = (local_out + carried_out).reshape(users, STRETCH, inner_width)
        gated_rows = mixture * jax.nn.silu(gate_rows)
        normed = (gated_rows * lax.rsqrt(lax.optimization_barrier(jnp.mean(gated_rows * gated_rows, axis=-1, keepdims=True)) + 1.0) * norm_gain).astype(jnp.bfloat16)
        result = jnp.dot(normed.reshape(users * STRETCH, inner_width), w_out, preferred_element_type=jnp.float32).reshape(users, STRETCH, -1)
        result = (result * usable[..., None]).astype(jnp.bfloat16)
        tail_weight = jnp.exp(log_heads - log_heads[:, :, -1:]) * size_heads
        scaled_in = rounded(inward[:, None, :, :] * tail_weight[..., None])
        stretch_state = jnp.einsum('shun,suhp->shpn', scaled_in, signal_heads)
        new_state = jnp.exp(-log_heads[:, :, -1])[..., None, None] * state_now + stretch_state
        return ((new_state, projected[:, STRETCH - (kernel - 1):, :]), result)
    initial = (jnp.zeros((users, head_count, head_size, state_width), jnp.float32), jnp.zeros((users, kernel - 1, full_width), jnp.bfloat16))
    _, results = lax.scan(advance, initial, (item_stretches, mask_stretches, starts))
    return results.transpose(1, 0, 2, 3).reshape(item_ids.shape + (item_table.shape[1],))
```

```python
import functools

import jax
import jax.numpy as jnp
from jax import lax
from jax.experimental import pallas as pl
from jax.experimental.pallas import tpu as pltpu
from jax.sharding import PartitionSpec as P

STRETCH = 128
CHUNK = 256
HALO = 16
ROWS, YS, ZS = 4, 4, 8
MESH = pl.DeviceIdType.MESH
BF16 = jnp.bfloat16
F32 = jnp.float32


def silu(v):
    return v * (0.5 * jnp.tanh(0.5 * v) + 0.5)


def dot(a, b):
    return jnp.dot(a, b, preferred_element_type=F32)


def down_columns(row):
    return jnp.transpose(jnp.broadcast_to(row, (STRETCH, STRETCH)))


def local_kernel(
    lengths,
    ids,
    halo,
    pads,
    table,
    w_gate,
    w_in,
    w_dt,
    taps,
    bias,
    rates,
    state_out,
    logs_out,
    mix,
    gate,
    outward,
    decays,
    wdt_wide,
    bias_wide,
    rates_wide,
    hot,
    joined,
    signal,
    inward,
    steps,
    running,
    passed,
):
    users, _, events = ids.shape
    inner = w_gate.shape[1]
    heads = w_dt.shape[1]
    stretches = events // STRETCH
    first = (lax.axis_index("col") * ROWS + lax.axis_index("row")) * events
    lanes = lax.broadcasted_iota(jnp.int32, (STRETCH, STRETCH), 1)
    lanes_f = lanes.astype(F32)

    def one_hot(row, place, rows):
        column = down_columns(row)[STRETCH - rows :, :]
        for j in range(table.shape[0] // STRETCH):
            match = column == lanes_f[:rows] + float(j * STRETCH)
            hot[place[0], pl.ds(place[1], rows), j * STRETCH : (j + 1) * STRETCH] = jnp.where(
                match, 1.0, 0.0
            ).astype(BF16)

    for u in range(users):
        one_hot(halo[u].astype(F32) - 1.0, (u, 0), HALO)
        for c in range(stretches):
            one_hot(
                ids[u, :, c * STRETCH : (c + 1) * STRETCH].astype(F32),
                (u, HALO + c * STRETCH),
                STRETCH,
            )

    wdt_wide[...] = jnp.zeros_like(wdt_wide)
    wdt_wide[:, 0:heads] = w_dt[...]
    bias_wide[...] = jnp.zeros_like(bias_wide)
    bias_wide[:, 0:heads] = bias[...]
    rates_wide[...] = jnp.zeros_like(rates_wide)
    rates_wide[:, 0:heads] = rates[...]
    raw = dot(table[...], wdt_wide[...]) + bias_wide[...]
    soft = jnp.maximum(raw, 0.0) + jnp.log1p(jnp.exp(-jnp.abs(raw)))
    high = soft.astype(BF16)
    rest = soft - high.astype(F32)
    middle = rest.astype(BF16)
    low = (rest - middle.astype(F32)).astype(BF16)
    for u in range(users):
        picks = hot[u, HALO:, :]
        step = dot(picks, high) + (dot(picks, middle) + dot(picks, low))
        for c in range(stretches):
            place = first + c * STRETCH + lax.broadcasted_iota(jnp.int32, (1, STRETCH), 1)
            kept = jnp.logical_and(
                place < lengths[u], pads[u, :, c * STRETCH : (c + 1) * STRETCH] > 0
            )
            usable = down_columns(jnp.where(kept, 1.0, 0.0))
            rows = slice(c * STRETCH, (c + 1) * STRETCH)
            steps[u, rows, :] = jnp.where(
                lanes == heads, usable, jnp.where(lanes < heads, step[rows] * usable, 0.0)
            )

    def project(j, weights):
        columns = pl.ds(pl.multiple_of(j * CHUNK, CHUNK), CHUNK)
        return columns, dot(table[...], weights[:, columns]).astype(BF16)

    def convolve(columns, projected, u):
        joined[u] = dot(hot[u], projected)
        total = None
        for k in range(taps.shape[0]):
            begin = HALO - taps.shape[0] + 1 + k
            term = joined[u, begin : begin + events, :] * taps[k : k + 1, columns]
            total = term if total is None else total + term
        return total

    @pl.loop(0, inner // CHUNK)
    def _(j):
        columns, projected = project(j, w_in)
        for u in range(users):
            signal[u, :, columns] = silu(convolve(columns, projected, u)).astype(BF16)
        columns, projected = project(j, w_gate)
        opened = silu(projected.astype(F32)).astype(BF16)
        for u in range(users):
            gate[u, :, columns] = dot(hot[u, HALO:, :], opened).astype(BF16)

    columns, projected = project(inner // CHUNK, w_in)
    for u in range(users):
        maps = convolve(columns, projected, u).astype(BF16)
        inward[u] = maps[:, 0:STRETCH]
        outward[u] = maps[:, STRETCH:]

    causal = lax.broadcasted_iota(jnp.int32, (STRETCH, STRETCH), 0) >= lanes
    lower = jnp.where(causal, 1.0, 0.0)
    running[...] = jnp.zeros_like(running)
    passed[...] = jnp.zeros_like(passed)

    @pl.loop(0, users * stretches)
    def _(s):
        u = s // stretches
        c = lax.rem(s, stretches)
        rows = pl.ds(pl.multiple_of(c * STRETCH, STRETCH), STRETCH)
        opening = c == 0
        step = steps[u, rows, :]
        log = jnp.dot(
            lower,
            step * rates_wide[...],
            preferred_element_type=F32,
            precision=lax.Precision.HIGHEST,
        )
        before = jnp.where(opening, 0.0, passed[...])
        decays[u, rows, :] = jnp.where(lanes == heads, step, jnp.exp(-(log + before)))
        passed[...] = before + log[STRETCH - 1 :, :]
        fade = jnp.exp(-log)
        log_t = jnp.transpose(log)[0:heads]
        step_t = jnp.transpose(step)[0:heads]
        last = log_t[:, STRETCH - 1 :]
        tail_t = jnp.exp(log_t - last) * step_t
        stay = jnp.exp(-last)
        ins = inward[u, rows, :]
        outs = outward[u, rows, :]
        in_t = jnp.transpose(ins.astype(F32))
        scores = lax.dot_general(outs, ins, (((1,), (1,)), ((), ())), preferred_element_type=F32)
        for h in range(heads):
            cols = slice(h * STRETCH, (h + 1) * STRETCH)
            inside = jnp.where(opening, 0.0, running[:, cols])
            gap = jnp.where(causal, log_t[h : h + 1, :] - log[:, h : h + 1], -1e30)
            weights = (scores * jnp.exp(gap) * step_t[h : h + 1, :]).astype(BF16)
            values = signal[u, rows, cols]
            mix[u, rows, cols] = (
                dot(weights, values) + dot(outs, inside.astype(BF16)) * fade[:, h : h + 1]
            ).astype(BF16)
            scaled = (in_t * tail_t[h : h + 1, :]).astype(BF16)
            running[:, cols] = stay[h : h + 1, :] * inside + dot(scaled, values)

        @pl.when(c == stretches - 1)
        def _():
            for h in range(heads):
                r, half = h // 2, h % 2
                cols = slice(half * STRETCH, (half + 1) * STRETCH)
                state_out[r, u, :, cols] = running[:, h * STRETCH : (h + 1) * STRETCH].astype(BF16)
                logs_out[r, u, :, cols] = jnp.broadcast_to(passed[:, h : h + 1], (1, STRETCH))


def scan_kernel(
    states,
    logs,
    carry,
    row_states,
    row_logs,
    row_before,
    z_out,
    z_states,
    z_log_out,
    z_logs,
    y_out,
    y_states,
    y_log_out,
    y_logs,
    c_out,
    c_states,
    back_out,
    x_send,
    x_recv,
    xl_send,
    xl_recv,
    z_send,
    z_recv,
    zl_send,
    zl_recv,
    y_send,
    y_recv,
    yl_send,
    yl_recv,
    c_send,
    c_recv,
    b_send,
    b_recv,
):
    users = states.shape[1]
    part = z_states.shape[2]
    r = lax.axis_index("row")
    col = lax.axis_index("col")
    y, z = col // ZS, lax.rem(col, ZS)

    def row_peer(d):
        return lax.rem(r + d, ROWS)

    def z_peer(d):
        return lax.rem(z + d, ZS)

    def y_peer(d):
        return lax.rem(y + d, YS)

    def to_row(d):
        return {"row": row_peer(d)}

    def to_z(d):
        return {"col": y * ZS + z_peer(d)}

    def to_y(d):
        return {"col": y_peer(d) * ZS + z}

    barrier = pltpu.get_barrier_semaphore()
    peers = (
        [to_row(d) for d in range(1, ROWS)]
        + [to_z(d) for d in range(1, ZS)]
        + [to_y(d) for d in range(1, YS)]
    )
    for peer in peers:
        pl.semaphore_signal(barrier, inc=1, device_id=peer, device_id_type=MESH)
    pl.semaphore_wait(barrier, len(peers))

    sent = []

    def send(src, dst, send_sem, recv_sem, device):
        copy = pltpu.make_async_remote_copy(
            src_ref=src,
            dst_ref=dst,
            send_sem=send_sem,
            recv_sem=recv_sem,
            device_id=device,
            device_id_type=MESH,
        )
        copy.start()
        sent.append(copy)
        return copy

    x_copies, xl_copies = {}, {}
    for d in (2, 1, 3):
        xl_copies[d] = send(
            logs.at[row_peer(d)], row_logs.at[r], xl_send.at[d], xl_recv.at[d], to_row(d)
        )
    for u in range(users):
        for d in (2, 1, 3):
            x_copies[u, d] = send(
                states.at[row_peer(d), u],
                row_states.at[u, r],
                x_send.at[u, d],
                x_recv.at[u, d],
                to_row(d),
            )
    row_logs[r] = logs[r]
    for u in range(users):
        row_states[u, r] = states[r, u]

    for d in range(1, ROWS):
        xl_copies[d].wait_recv()
    block_log = row_logs[0]
    for i in range(1, ROWS):
        block_log = block_log + row_logs[i]
    z_log_out[...] = block_log
    z_logs[z] = block_log
    zl_copies = [
        send(z_log_out, z_logs.at[z], zl_send.at[d], zl_recv.at[d], to_z(d)) for d in range(1, ZS)
    ]

    z_copies = {}
    for u in range(users):
        for d in range(1, ROWS):
            x_copies[u, d].wait_recv()
        total = row_states[u, 0].astype(F32)
        for i in range(1, ROWS):
            row_before[u, i - 1] = total
            total = jnp.exp(-row_logs[i, u]) * total + row_states[u, i].astype(F32)
        block = total.astype(BF16)
        for k in range(ZS):
            z_out[u, k] = block[k * part : (k + 1) * part]
        z_states[u, z] = z_out[u, z]
        for d in (4, 3, 5, 2, 6, 1, 7):
            z_copies[u, d] = send(
                z_out.at[u, z_peer(d)],
                z_states.at[u, z],
                z_send.at[u, d],
                z_recv.at[u, d],
                to_z(d),
            )

    for copy in zl_copies:
        copy.wait_recv()
    y_log = z_logs[0]
    for i in range(1, ZS):
        y_log = y_log + z_logs[i]
    y_log_out[...] = y_log
    y_logs[y] = y_log
    yl_copies = [
        send(y_log_out, y_logs.at[y], yl_send.at[d], yl_recv.at[d], to_y(d)) for d in range(1, YS)
    ]

    y_copies, z_before = {}, {}
    for u in range(users):
        for d in range(1, ZS):
            z_copies[u, d].wait_recv()
        z_before[u] = [None]
        total = z_states[u, 0].astype(F32)
        for i in range(1, ZS):
            z_before[u].append(total)
            total = jnp.exp(-z_logs[i, u]) * total + z_states[u, i].astype(F32)
        y_out[u] = total.astype(BF16)
        for d in (2, 1, 3):
            y_copies[u, d] = send(
                y_out.at[u], y_states.at[u, y], y_send.at[u, d], y_recv.at[u, d], to_y(d)
            )

    for copy in yl_copies:
        copy.wait_recv()
    c_copies = {}
    for u in range(users):
        for d in range(1, YS):
            y_copies[u, d].wait_recv()
        y_states[u, y] = jnp.zeros_like(y_states[u, y])
        entering = jnp.zeros(y_out.shape[1:], F32)
        for i in range(YS - 1):
            entering = jnp.where(
                i < y, jnp.exp(-y_logs[i, u]) * entering + y_states[u, i].astype(F32), entering
            )
        gone = None
        for k in range(ZS):
            value = entering
            if k:
                gone = z_logs[k - 1, u] if gone is None else gone + z_logs[k - 1, u]
                value = jnp.exp(-gone) * entering + z_before[u][k]
            c_out[u, k] = value.astype(BF16)
        c_states[u, z] = c_out[u, z]
        for d in (4, 3, 5, 2, 6, 1, 7):
            c_copies[u, d] = send(
                c_out.at[u, z_peer(d)],
                c_states.at[u, z],
                c_send.at[u, d],
                c_recv.at[u, d],
                to_z(d),
            )

    b_copies = {}
    for u in range(users):
        for d in range(1, ZS):
            c_copies[u, d].wait_recv()
        gone = None
        for i in range(ROWS):
            if i:
                gone = row_logs[i - 1, u] if gone is None else gone + row_logs[i - 1, u]
            for k in range(ZS):
                rows = slice(k * part, (k + 1) * part)
                value = c_states[u, k].astype(F32)
                if i:
                    value = jnp.exp(-gone) * value + row_before[u, i - 1, rows, :]
                back_out[u, i, rows, :] = value.astype(BF16)
        carry[u, r] = back_out[u, r]
        for d in (2, 1, 3):
            b_copies[u, d] = send(
                back_out.at[u, row_peer(d)],
                carry.at[u, r],
                b_send.at[u, d],
                b_recv.at[u, d],
                to_row(d),
            )
    for copy in b_copies.values():
        copy.wait_recv()
    for copy in sent:
        copy.wait_send()


def final_kernel(carry, mix, gate, outward, decays, gain, w_out, result, gated, normed):
    inner = mix.shape[2]
    heads = inner // STRETCH
    events = mix.shape[1]

    @pl.loop(0, events // STRETCH)
    def _(c):
        rows = pl.ds(pl.multiple_of(c * STRETCH, STRETCH), STRETCH)
        outs = outward[0, rows, :]
        squares = jnp.zeros((STRETCH, STRETCH), F32)
        for r in range(ROWS):
            carried = dot(outs, carry[0, r])
            for half in range(2):
                h = 2 * r + half
                cols = slice(h * STRETCH, (h + 1) * STRETCH)
                value = mix[0, rows, cols].astype(F32) + decays[0, rows, h : h + 1] * carried[
                    :, half * STRETCH : (half + 1) * STRETCH
                ]
                value = value * gate[0, rows, cols].astype(F32)
                squares = squares + value * value
                gated[:, cols] = value
        mean = jnp.sum(squares, axis=1, keepdims=True) * (1.0 / inner)
        scale = lax.rsqrt(mean + 1.0)
        for h in range(heads):
            cols = slice(h * STRETCH, (h + 1) * STRETCH)
            normed[rows, cols] = (gated[:, cols] * scale * gain[:, cols]).astype(BF16)

    usable = decays[0, :, heads : heads + 1]

    @pl.loop(0, w_out.shape[1] // CHUNK)
    def _(j):
        columns = pl.ds(pl.multiple_of(j * CHUNK, CHUNK), CHUNK)
        result[0, 0, :, columns] = (dot(normed[...], w_out[:, columns]) * usable).astype(BF16)


def per_device(
    item_ids,
    pad_masks,
    lengths,
    item_table,
    w_gate,
    w_in,
    w_dt,
    conv_taps,
    dt_bias,
    decay_rates,
    norm_gain,
    w_out,
):
    users, _, events = item_ids.shape
    inner = w_gate.shape[1]
    heads = decay_rates.shape[0]
    pair = 2 * STRETCH
    cols = lax.axis_size("col")
    route = [(r * cols + c, (r + 1) * cols + c) for r in range(ROWS - 1) for c in range(cols)]
    route += [((ROWS - 1) * cols + c, c + 1) for c in range(cols - 1)]
    ids_behind = lax.ppermute(
        item_ids[:, :, events - STRETCH :] + 1, ("row", "col"), route
    )
    vmem = pl.BlockSpec(memory_space=pltpu.VMEM)
    states, logs, mix, gate, outward, decays = pl.pallas_call(
        local_kernel,
        name="local",
        out_shape=(
            jax.ShapeDtypeStruct((ROWS, users, STRETCH, pair), BF16),
            jax.ShapeDtypeStruct((ROWS, users, 1, pair), F32),
            jax.ShapeDtypeStruct((users, events, inner), BF16),
            jax.ShapeDtypeStruct((users, events, inner), BF16),
            jax.ShapeDtypeStruct((users, events, STRETCH), BF16),
            jax.ShapeDtypeStruct((users, events, STRETCH), F32),
        ),
        in_specs=[pl.BlockSpec(memory_space=pltpu.SMEM)] + [vmem] * 10,
        out_specs=(vmem,) * 6,
        scratch_shapes=[
            pltpu.VMEM((inner, STRETCH), BF16),
            pltpu.VMEM((1, STRETCH), F32),
            pltpu.VMEM((1, STRETCH), F32),
            pltpu.VMEM((users, HALO + events, item_table.shape[0]), BF16),
            pltpu.VMEM((users, HALO + events, CHUNK), F32),
            pltpu.VMEM((users, events, inner), BF16),
            pltpu.VMEM((users, events, STRETCH), BF16),
            pltpu.VMEM((users, events, STRETCH), F32),
            pltpu.VMEM((STRETCH, inner), F32),
            pltpu.VMEM((1, STRETCH), F32),
        ],
    )(
        lengths,
        item_ids,
        ids_behind,
        pad_masks,
        item_table,
        w_gate,
        w_in,
        w_dt,
        conv_taps,
        dt_bias.reshape(1, heads),
        decay_rates.reshape(1, heads),
    )
    part = STRETCH // ZS
    dma = pltpu.SemaphoreType.DMA
    carry = pl.pallas_call(
        scan_kernel,
        name="scan",
        out_shape=jax.ShapeDtypeStruct((users, ROWS, STRETCH, pair), BF16),
        in_specs=[vmem] * 2,
        out_specs=vmem,
        scratch_shapes=[
            pltpu.VMEM((users, ROWS, STRETCH, pair), BF16),
            pltpu.VMEM((ROWS, users, 1, pair), F32),
            pltpu.VMEM((users, ROWS - 1, STRETCH, pair), F32),
            pltpu.VMEM((users, ZS, part, pair), BF16),
            pltpu.VMEM((users, ZS, part, pair), BF16),
            pltpu.VMEM((users, 1, pair), F32),
            pltpu.VMEM((ZS, users, 1, pair), F32),
            pltpu.VMEM((users, part, pair), BF16),
            pltpu.VMEM((users, YS, part, pair), BF16),
            pltpu.VMEM((users, 1, pair), F32),
            pltpu.VMEM((YS, users, 1, pair), F32),
            pltpu.VMEM((users, ZS, part, pair), BF16),
            pltpu.VMEM((users, ZS, part, pair), BF16),
            pltpu.VMEM((users, ROWS, STRETCH, pair), BF16),
            dma((users, ROWS)),
            dma((users, ROWS)),
            dma((ROWS,)),
            dma((ROWS,)),
            dma((users, ZS)),
            dma((users, ZS)),
            dma((ZS,)),
            dma((ZS,)),
            dma((users, YS)),
            dma((users, YS)),
            dma((YS,)),
            dma((YS,)),
            dma((users, ZS)),
            dma((users, ZS)),
            dma((users, ROWS)),
            dma((users, ROWS)),
        ],
        compiler_params=pltpu.CompilerParams(collective_id=0, has_side_effects=True),
    )(states, logs)
    by_user = lambda *shape: pl.BlockSpec((1, *shape), lambda u: (u,) + (0,) * len(shape))
    return pl.pallas_call(
        final_kernel,
        name="final",
        grid=(users,),
        out_shape=jax.ShapeDtypeStruct((users, 1, events, w_out.shape[1]), BF16),
        in_specs=[
            by_user(ROWS, STRETCH, pair),
            by_user(events, inner),
            by_user(events, inner),
            by_user(events, STRETCH),
            by_user(events, STRETCH),
            pl.BlockSpec((1, inner), lambda u: (0, 0)),
            pl.BlockSpec(w_out.shape, lambda u: (0, 0)),
        ],
        out_specs=by_user(1, events, w_out.shape[1]),
        scratch_shapes=[pltpu.VMEM((STRETCH, inner), F32), pltpu.VMEM((events, inner), BF16)],
    )(carry, mix, gate, outward, decays, norm_gain.reshape(1, inner), w_out)


def solution(mesh):
    spans = P("batch", "col", "row")
    return jax.shard_map(
        per_device,
        mesh=mesh,
        in_specs=(spans, spans, P("batch")) + (P(),) * 9,
        out_specs=P("batch", "col", "row", None),
        check_vma=False,
    )
```

```python
import jax
import jax.numpy as jnp
from jax import lax
from jax.experimental import pallas as pl
from jax.experimental.pallas import tpu as pltpu
from jax.sharding import PartitionSpec as P

STRETCH = 128
CHUNK = 256
HALO = 16
ROWS, YS, ZS = 4, 4, 8
MESH = pl.DeviceIdType.MESH
BF16 = jnp.bfloat16
F32 = jnp.float32


def silu(v):
    return v * (0.5 * jnp.tanh(0.5 * v) + 0.5)


def dot(a, b):
    return jnp.dot(a, b, preferred_element_type=F32)


def down_columns(row):
    return jnp.transpose(jnp.broadcast_to(row, (STRETCH, STRETCH)))


def main_kernel(
    lengths,
    ids,
    pads,
    w_dt,
    taps,
    bias,
    rates,
    table_in,
    w_in_in,
    w_gate_in,
    carry,
    mix,
    gate,
    outward,
    decays,
    table,
    w_in,
    w_gate,
    wdt_wide,
    bias_wide,
    rates_wide,
    split_steps,
    halo,
    hot,
    projected,
    joined_even,
    joined_odd,
    signal,
    inward,
    steps,
    log_columns,
    log_rows,
    step_rows,
    inside,
    running,
    passed,
    states,
    logs,
    row_states,
    row_logs,
    row_before,
    z_out,
    z_states,
    z_before,
    z_log_out,
    z_logs,
    y_out,
    y_states,
    y_log_out,
    y_logs,
    c_out,
    c_states,
    back_out,
    load_sem,
    halo_send,
    halo_recv,
    x_send,
    x_recv,
    xl_send,
    xl_recv,
    z_send,
    z_recv,
    zl_send,
    zl_recv,
    y_send,
    y_recv,
    yl_send,
    yl_recv,
    c_send,
    c_recv,
    b_send,
    b_recv,
):
    users, _, events = ids.shape
    inner = w_gate.shape[1]
    heads = w_dt.shape[0]
    stretches = events // STRETCH
    chunks = w_in.shape[1] // CHUNK
    part = z_states.shape[2]
    r = lax.axis_index("row")
    col = lax.axis_index("col")
    cols_axis = lax.axis_size("col")
    y, z = col // ZS, lax.rem(col, ZS)
    first = (col * ROWS + r) * events

    loads = [pltpu.make_async_copy(table_in, table, load_sem.at[0])]
    for j in range(chunks):
        columns = slice(j * CHUNK, (j + 1) * CHUNK)
        loads.append(
            pltpu.make_async_copy(w_in_in.at[:, columns], w_in.at[:, columns], load_sem.at[1 + j])
        )
    loads.append(pltpu.make_async_copy(w_gate_in, w_gate, load_sem.at[1 + chunks]))
    for load in loads:
        load.start()

    def row_peer(d):
        return lax.rem(r + d, ROWS)

    def z_peer(d):
        return lax.rem(z + d, ZS)

    def to_row(d):
        return {"row": row_peer(d)}

    def to_z(d):
        return {"col": y * ZS + z_peer(d)}

    def to_y(d):
        return {"col": lax.rem(y + d, YS) * ZS + z}

    next_span = {
        "row": row_peer(1),
        "col": lax.rem(col + jnp.where(r == ROWS - 1, 1, 0), cols_axis),
    }
    last_span = {
        "row": row_peer(ROWS - 1),
        "col": lax.rem(col + jnp.where(r == 0, cols_axis - 1, 0), cols_axis),
    }
    barrier = pltpu.get_barrier_semaphore()
    peers = (
        [to_row(d) for d in range(1, ROWS)]
        + [to_z(d) for d in range(1, ZS)]
        + [to_y(d) for d in range(1, YS)]
        + [next_span, last_span]
    )
    for peer in peers:
        pl.semaphore_signal(barrier, inc=1, device_id=peer, device_id_type=MESH)

    sent = []

    def send(src, dst, send_sem, recv_sem, device):
        copy = pltpu.make_async_remote_copy(
            src_ref=src,
            dst_ref=dst,
            send_sem=send_sem,
            recv_sem=recv_sem,
            device_id=device,
            device_id_type=MESH,
        )
        copy.start()
        sent.append(copy)
        return copy

    lanes = lax.broadcasted_iota(jnp.int32, (STRETCH, STRETCH), 1)
    lanes_f = lanes.astype(F32)
    causal = lax.broadcasted_iota(jnp.int32, (STRETCH, STRETCH), 0) >= lanes

    def one_hot(row, u, begin, rows):
        column = down_columns(row)[STRETCH - rows :, :]
        for j in range(table.shape[0] // STRETCH):
            match = column == lanes_f[:rows] + float(j * STRETCH)
            hot[u, begin : begin + rows, j * STRETCH : (j + 1) * STRETCH] = jnp.where(
                match, 1.0, 0.0
            ).astype(BF16)

    for u in range(users):
        for c in range(stretches):
            row = ids[u, :, c * STRETCH : (c + 1) * STRETCH].astype(F32)
            one_hot(row, u, HALO + c * STRETCH, STRETCH)
    wdt_wide[...] = jnp.zeros_like(wdt_wide)
    wdt_wide[0:heads, :] = w_dt[...]
    bias_wide[...] = jnp.zeros_like(bias_wide)
    bias_wide[:, 0:heads] = bias[...]
    rates_wide[...] = jnp.zeros_like(rates_wide)
    rates_wide[:, 0:heads] = rates[...]

    pl.semaphore_wait(barrier, len(peers))
    tail = slice(events - STRETCH, events)
    halo_copy = send(ids.at[:, :, tail], halo, halo_send, halo_recv, next_span)

    loads[0].wait()
    raw = lax.dot_general(
        table[...], wdt_wide[...], (((1,), (1,)), ((), ())), preferred_element_type=F32
    )
    raw = raw + bias_wide[...]
    soft = jnp.maximum(raw, 0.0) + jnp.log1p(jnp.exp(-jnp.abs(raw)))
    high = soft.astype(BF16)
    rest = soft - high.astype(F32)
    middle = rest.astype(BF16)
    split_steps[:, 0:STRETCH] = high
    split_steps[:, STRETCH : 2 * STRETCH] = middle
    split_steps[:, 2 * STRETCH :] = (rest - middle.astype(F32)).astype(BF16)
    for u in range(users):
        picked = dot(hot[u, HALO:, :], split_steps[...])
        step = picked[:, 0:STRETCH] + (
            picked[:, STRETCH : 2 * STRETCH] + picked[:, 2 * STRETCH :]
        )
        for c in range(stretches):
            place = first + c * STRETCH + lax.broadcasted_iota(jnp.int32, (1, STRETCH), 1)
            rows = slice(c * STRETCH, (c + 1) * STRETCH)
            kept = jnp.logical_and(place < lengths[u], pads[u, :, rows] > 0)
            usable = down_columns(jnp.where(kept, 1.0, 0.0))
            steps[u, rows, :] = jnp.where(
                lanes == heads, usable, jnp.where(lanes < heads, step[rows] * usable, 0.0)
            )

    for j in range(chunks):
        columns = slice(j * CHUNK, (j + 1) * CHUNK)
        loads[1 + j].wait()
        projected[:, columns] = dot(table[...], w_in[:, columns]).astype(BF16)

    halo_copy.wait_recv()
    nobody = jnp.logical_and(r == 0, col == 0)
    for u in range(users):
        one_hot(jnp.where(nobody, -1.0, halo[u].astype(F32)), u, 0, HALO)

    joined = (joined_even, joined_odd)

    def gather(u, j):
        joined[j % 2][...] = dot(hot[u], projected[:, j * CHUNK : (j + 1) * CHUNK])

    def convolve(u, j):
        columns = slice(j * CHUNK, (j + 1) * CHUNK)
        total = None
        for k in range(taps.shape[0]):
            begin = HALO - taps.shape[0] + 1 + k
            term = joined[j % 2][begin : begin + events, :] * taps[k : k + 1, columns]
            total = term if total is None else total + term
        if j < chunks - 1:
            signal[u, :, columns] = silu(total).astype(BF16)
        else:
            maps = total.astype(BF16)
            inward[u] = maps[:, 0:STRETCH]
            outward[u] = maps[:, STRETCH:]

    def state_phase(u):
        gather(u, 0)
        for j in range(chunks):
            if j + 1 < chunks:
                gather(u, j + 1)
            convolve(u, j)
        lower = jnp.where(causal, 1.0, 0.0)
        passed[...] = jnp.zeros_like(passed)

        @pl.loop(0, stretches)
        def _(c):
            rows = pl.ds(pl.multiple_of(c * STRETCH, STRETCH), STRETCH)
            step = steps[u, rows, :]
            log = jnp.dot(
                lower,
                step * rates_wide[...],
                preferred_element_type=F32,
                precision=lax.Precision.HIGHEST,
            )
            before = passed[...]
            decays[u, rows, :] = jnp.where(lanes == heads, step, jnp.exp(-(log + before)))
            passed[...] = before + log[STRETCH - 1 :, :]
            log_columns[u, rows, :] = log
            log_t = jnp.transpose(log)[0:heads]
            step_t = jnp.transpose(step)[0:heads]
            log_rows[u, c] = log_t
            step_rows[u, c] = step_t
            last = log_t[:, STRETCH - 1 :]
            tail_t = jnp.exp(log_t - last) * step_t
            stay = jnp.exp(-last)
            in_t = jnp.transpose(inward[u, rows, :].astype(F32))
            for h in range(heads):
                cols = slice(h * STRETCH, (h + 1) * STRETCH)
                entering = jnp.where(c == 0, 0.0, running[:, cols])
                inside[u, c, :, cols] = entering.astype(BF16)
                scaled = (in_t * tail_t[h : h + 1, :]).astype(BF16)
                running[:, cols] = stay[h : h + 1, :] * entering + dot(
                    scaled, signal[u, rows, cols]
                )

        for h in range(heads):
            half = h % 2
            cols = slice(half * STRETCH, (half + 1) * STRETCH)
            states[h // 2, u, :, cols] = running[:, h * STRETCH : (h + 1) * STRETCH].astype(BF16)
            logs[h // 2, u, :, cols] = jnp.broadcast_to(passed[:, h : h + 1], (1, STRETCH))

    def local_phase(u, begin, end):
        @pl.loop(begin, end)
        def _(c):
            rows = pl.ds(pl.multiple_of(c * STRETCH, STRETCH), STRETCH)
            log = log_columns[u, rows, :]
            fade = jnp.exp(-log)
            log_t = log_rows[u, c]
            step_t = step_rows[u, c]
            outs = outward[u, rows, :]
            scores = lax.dot_general(
                outs, inward[u, rows, :], (((1,), (1,)), ((), ())), preferred_element_type=F32
            )
            for h in range(heads):
                cols = slice(h * STRETCH, (h + 1) * STRETCH)
                gap = jnp.where(causal, log_t[h : h + 1, :] - log[:, h : h + 1], -1e30)
                weights = (scores * jnp.exp(gap) * step_t[h : h + 1, :]).astype(BF16)
                mix[u, rows, cols] = (
                    dot(weights, signal[u, rows, cols])
                    + dot(outs, inside[u, c, :, cols]) * fade[:, h : h + 1]
                ).astype(BF16)

    x_copies, xl_copies, z_copies, y_copies, c_copies, b_copies = {}, {}, {}, {}, {}, {}
    for u in range(users):
        state_phase(u)
        for d in (2, 1, 3):
            xl_copies[u, d] = send(
                logs.at[row_peer(d), u],
                row_logs.at[u, r],
                xl_send.at[u, d],
                xl_recv.at[u, d],
                to_row(d),
            )
            x_copies[u, d] = send(
                states.at[row_peer(d), u],
                row_states.at[u, r],
                x_send.at[u, d],
                x_recv.at[u, d],
                to_row(d),
            )
        row_logs[u, r] = logs[r, u]
        row_states[u, r] = states[r, u]

    def row_step(u):
        for d in range(1, ROWS):
            xl_copies[u, d].wait_recv()
            x_copies[u, d].wait_recv()
        block_log = row_logs[u, 0]
        for i in range(1, ROWS):
            block_log = block_log + row_logs[u, i]
        z_log_out[u] = block_log
        z_logs[u, z] = block_log
        total = row_states[u, 0].astype(F32)
        for i in range(1, ROWS):
            row_before[u, i - 1] = total
            total = jnp.exp(-row_logs[u, i]) * total + row_states[u, i].astype(F32)
        block = total.astype(BF16)
        for k in range(ZS):
            z_out[u, k] = block[k * part : (k + 1) * part]
        z_states[u, z] = z_out[u, z]
        for d in (4, 3, 5, 2, 6, 1, 7):
            z_copies[u, d] = (
                send(
                    z_log_out.at[u], z_logs.at[u, z], zl_send.at[u, d], zl_recv.at[u, d], to_z(d)
                ),
                send(
                    z_out.at[u, z_peer(d)],
                    z_states.at[u, z],
                    z_send.at[u, d],
                    z_recv.at[u, d],
                    to_z(d),
                ),
            )

    def z_step(u):
        for d in range(1, ZS):
            for copy in z_copies[u, d]:
                copy.wait_recv()
        y_log = z_logs[u, 0]
        for i in range(1, ZS):
            y_log = y_log + z_logs[u, i]
        y_log_out[u] = y_log
        y_logs[u, y] = y_log
        total = z_states[u, 0].astype(F32)
        for i in range(1, ZS):
            z_before[u, i - 1] = total
            total = jnp.exp(-z_logs[u, i]) * total + z_states[u, i].astype(F32)
        y_out[u] = total.astype(BF16)
        for d in (2, 1, 3):
            y_copies[u, d] = (
                send(
                    y_log_out.at[u], y_logs.at[u, y], yl_send.at[u, d], yl_recv.at[u, d], to_y(d)
                ),
                send(y_out.at[u], y_states.at[u, y], y_send.at[u, d], y_recv.at[u, d], to_y(d)),
            )

    def y_step(u):
        for d in range(1, YS):
            for copy in y_copies[u, d]:
                copy.wait_recv()
        entering = jnp.zeros(y_out.shape[1:], F32)
        for i in range(YS - 1):
            entering = jnp.where(
                i < y, jnp.exp(-y_logs[u, i]) * entering + y_states[u, i].astype(F32), entering
            )
        gone = None
        for k in range(ZS):
            value = entering
            if k:
                gone = z_logs[u, k - 1] if gone is None else gone + z_logs[u, k - 1]
                value = jnp.exp(-gone) * entering + z_before[u, k - 1]
            c_out[u, k] = value.astype(BF16)
        c_states[u, z] = c_out[u, z]
        for d in (4, 3, 5, 2, 6, 1, 7):
            c_copies[u, d] = send(
                c_out.at[u, z_peer(d)],
                c_states.at[u, z],
                c_send.at[u, d],
                c_recv.at[u, d],
                to_z(d),
            )

    def back_step(u):
        for d in range(1, ZS):
            c_copies[u, d].wait_recv()
        gone = None
        for i in range(ROWS):
            if i:
                gone = row_logs[u, i - 1] if gone is None else gone + row_logs[u, i - 1]
            for k in range(ZS):
                rows = slice(k * part, (k + 1) * part)
                value = c_states[u, k].astype(F32)
                if i:
                    value = jnp.exp(-gone) * value + row_before[u, i - 1, rows, :]
                back_out[u, i, rows, :] = value.astype(BF16)
        carry[u, r] = back_out[u, r]
        for d in (2, 1, 3):
            b_copies[u, d] = send(
                back_out.at[u, row_peer(d)],
                carry.at[u, r],
                b_send.at[u, d],
                b_recv.at[u, d],
                to_row(d),
            )

    loads[-1].wait()

    @pl.loop(0, inner // CHUNK)
    def _(j):
        columns = pl.ds(pl.multiple_of(j * CHUNK, CHUNK), CHUNK)
        opened = dot(table[...], w_gate[:, columns]).astype(BF16)
        opened = silu(opened.astype(F32)).astype(BF16)
        for u in range(users):
            gate[u, :, columns] = dot(hot[u, HALO:, :], opened).astype(BF16)

    half = stretches // 2
    row_step(0)
    local_phase(0, 0, half)
    row_step(1)
    local_phase(0, half, stretches)
    z_step(0)
    z_step(1)
    local_phase(1, 0, half)
    y_step(0)
    y_step(1)
    local_phase(1, half, stretches)
    back_step(0)
    back_step(1)
    for copy in b_copies.values():
        copy.wait_recv()
    for copy in sent:
        copy.wait_send()


def final_kernel(carry, mix, gate, outward, decays, gain, w_out, result, gated, normed, done, sems):
    users, events, inner = mix.shape
    heads = inner // STRETCH
    width = w_out.shape[1]

    def norm(u, c):
        rows = slice(c * STRETCH, (c + 1) * STRETCH)
        outs = outward[u, rows, :]
        squares = jnp.zeros((STRETCH, STRETCH), F32)
        for r in range(ROWS):
            carried = dot(outs, carry[u, r])
            for half in range(2):
                h = 2 * r + half
                cols = slice(h * STRETCH, (h + 1) * STRETCH)
                value = mix[u, rows, cols].astype(F32) + decays[u, rows, h : h + 1] * carried[
                    :, half * STRETCH : (half + 1) * STRETCH
                ]
                value = value * gate[u, rows, cols].astype(F32)
                squares = squares + value * value
                gated[c % 2, :, cols] = value
        mean = jnp.sum(squares, axis=1, keepdims=True) * (1.0 / inner)
        scale = lax.rsqrt(mean + 1.0)
        for h in range(heads):
            cols = slice(h * STRETCH, (h + 1) * STRETCH)
            normed[u, rows, cols] = (gated[c % 2, :, cols] * scale * gain[:, cols]).astype(BF16)

    copies = []

    def project(u, j):
        columns = slice(j * CHUNK, (j + 1) * CHUNK)
        usable = decays[u, :, heads : heads + 1]
        done[u, :, columns] = (dot(normed[u], w_out[:, columns]) * usable).astype(BF16)
        return columns

    def store(u, j, columns):
        copy = pltpu.make_async_copy(
            done.at[u, :, columns], result.at[u, 0, :, columns], sems.at[u, j]
        )
        copy.start()
        copies.append(copy)

    blocks = events // STRETCH
    for c in range(blocks):
        norm(0, c)
    for u in range(users):
        for j in range(width // CHUNK):
            columns = project(u, j)
            if u + 1 < users and j < blocks:
                norm(u + 1, j)
            store(u, j, columns)
    for copy in copies:
        copy.wait()


def per_device(
    item_ids,
    pad_masks,
    lengths,
    item_table,
    w_gate,
    w_in,
    w_dt,
    conv_taps,
    dt_bias,
    decay_rates,
    norm_gain,
    w_out,
):
    users, _, events = item_ids.shape
    items, width = item_table.shape
    inner = w_gate.shape[1]
    full = w_in.shape[1]
    heads = decay_rates.shape[0]
    stretches = events // STRETCH
    pair = 2 * STRETCH
    part = STRETCH // ZS
    vmem = pl.BlockSpec(memory_space=pltpu.VMEM)
    hbm = pl.BlockSpec(memory_space=pltpu.HBM)
    dma = pltpu.SemaphoreType.DMA
    carry, mix, gate, outward, decays = pl.pallas_call(
        main_kernel,
        name="main",
        out_shape=(
            jax.ShapeDtypeStruct((users, ROWS, STRETCH, pair), BF16),
            jax.ShapeDtypeStruct((users, events, inner), BF16),
            jax.ShapeDtypeStruct((users, events, inner), BF16),
            jax.ShapeDtypeStruct((users, events, STRETCH), BF16),
            jax.ShapeDtypeStruct((users, events, STRETCH), F32),
        ),
        in_specs=[pl.BlockSpec(memory_space=pltpu.SMEM)] + [vmem] * 6 + [hbm] * 3,
        out_specs=(vmem,) * 5,
        scratch_shapes=[
            pltpu.VMEM((items, width), BF16),
            pltpu.VMEM((width, full), BF16),
            pltpu.VMEM((width, inner), BF16),
            pltpu.VMEM((STRETCH, width), BF16),
            pltpu.VMEM((1, STRETCH), F32),
            pltpu.VMEM((1, STRETCH), F32),
            pltpu.VMEM((items, 3 * STRETCH), BF16),
            pltpu.VMEM((users, 1, STRETCH), jnp.int32),
            pltpu.VMEM((users, HALO + events, items), BF16),
            pltpu.VMEM((items, full), BF16),
            pltpu.VMEM((HALO + events, CHUNK), F32),
            pltpu.VMEM((HALO + events, CHUNK), F32),
            pltpu.VMEM((users, events, inner), BF16),
            pltpu.VMEM((users, events, STRETCH), BF16),
            pltpu.VMEM((users, events, STRETCH), F32),
            pltpu.VMEM((users, events, STRETCH), F32),
            pltpu.VMEM((users, stretches, heads, STRETCH), F32),
            pltpu.VMEM((users, stretches, heads, STRETCH), F32),
            pltpu.VMEM((users, stretches, STRETCH, inner), BF16),
            pltpu.VMEM((STRETCH, inner), F32),
            pltpu.VMEM((1, STRETCH), F32),
            pltpu.VMEM((ROWS, users, STRETCH, pair), BF16),
            pltpu.VMEM((ROWS, users, 1, pair), F32),
            pltpu.VMEM((users, ROWS, STRETCH, pair), BF16),
            pltpu.VMEM((users, ROWS, 1, pair), F32),
            pltpu.VMEM((users, ROWS - 1, STRETCH, pair), F32),
            pltpu.VMEM((users, ZS, part, pair), BF16),
            pltpu.VMEM((users, ZS, part, pair), BF16),
            pltpu.VMEM((users, ZS - 1, part, pair), F32),
            pltpu.VMEM((users, 1, pair), F32),
            pltpu.VMEM((users, ZS, 1, pair), F32),
            pltpu.VMEM((users, part, pair), BF16),
            pltpu.VMEM((users, YS, part, pair), BF16),
            pltpu.VMEM((users, 1, pair), F32),
            pltpu.VMEM((users, YS, 1, pair), F32),
            pltpu.VMEM((users, ZS, part, pair), BF16),
            pltpu.VMEM((users, ZS, part, pair), BF16),
            pltpu.VMEM((users, ROWS, STRETCH, pair), BF16),
            dma((2 + full // CHUNK,)),
            dma,
            dma,
        ]
        + [dma((users, ROWS))] * 4
        + [dma((users, ZS))] * 4
        + [dma((users, YS))] * 4
        + [dma((users, ZS))] * 2
        + [dma((users, ROWS))] * 2,
        compiler_params=pltpu.CompilerParams(
            collective_id=0, has_side_effects=True, vmem_limit_bytes=36 << 20
        ),
    )(
        lengths,
        item_ids,
        pad_masks,
        w_dt.T,
        conv_taps,
        dt_bias.reshape(1, heads),
        decay_rates.reshape(1, heads),
        item_table,
        w_in,
        w_gate,
    )
    return pl.pallas_call(
        final_kernel,
        name="final",
        out_shape=jax.ShapeDtypeStruct((users, 1, events, w_out.shape[1]), BF16),
        in_specs=[vmem] * 7,
        out_specs=hbm,
        scratch_shapes=[
            pltpu.VMEM((2, STRETCH, inner), F32),
            pltpu.VMEM((users, events, inner), BF16),
            pltpu.VMEM((users, events, w_out.shape[1]), BF16),
            dma((users, w_out.shape[1] // CHUNK)),
        ],
        compiler_params=pltpu.CompilerParams(vmem_limit_bytes=24 << 20),
    )(carry, mix, gate, outward, decays, norm_gain.reshape(1, inner), w_out)


def solution(mesh):
    spans = P("batch", "col", "row")
    return jax.shard_map(
        per_device,
        mesh=mesh,
        in_specs=(spans, spans, P("batch")) + (P(),) * 9,
        out_specs=P("batch", "col", "row", None),
        check_vma=False,
    )
```

```python
import jax
import jax.numpy as jnp
from jax import lax
from jax.experimental import pallas as pl
from jax.experimental.pallas import tpu as pltpu
from jax.sharding import PartitionSpec as P

STRETCH = 128
CHUNK = 256
HALO = 16
ROWS, YS, ZS = 4, 4, 8
MESH = pl.DeviceIdType.MESH
BF16 = jnp.bfloat16
F32 = jnp.float32


def silu(v):
    return v * (0.5 * jnp.tanh(0.5 * v) + 0.5)


def dot(a, b):
    return jnp.dot(a, b, preferred_element_type=F32)


def down_columns(row):
    return jnp.transpose(jnp.broadcast_to(row, (STRETCH, STRETCH)))


def main_kernel(
    lengths_in,
    ids_in,
    pads_in,
    w_dt_in,
    taps_in,
    bias_in,
    rates_in,
    table_in,
    w_in_in,
    w_gate_in,
    carry,
    mix,
    gate,
    outward,
    columns_out,
    lengths,
    ids,
    pads,
    w_dt,
    taps,
    bias,
    rates,
    table,
    w_in,
    w_gate,
    wdt_wide,
    split_steps,
    halo,
    hot,
    projected,
    joined_even,
    joined_odd,
    signal,
    inward,
    in_rows,
    slopes,
    log_rows,
    step_rows,
    tails,
    running,
    states,
    logs,
    row_states,
    row_logs,
    row_before,
    z_out,
    z_states,
    z_before,
    z_log_out,
    z_logs,
    y_out,
    y_states,
    y_log_out,
    y_logs,
    c_out,
    c_states,
    back_out,
    load_sem,
    halo_send,
    halo_recv,
    x_send,
    x_recv,
    xl_send,
    xl_recv,
    z_send,
    z_recv,
    zl_send,
    zl_recv,
    y_send,
    y_recv,
    yl_send,
    yl_recv,
    c_send,
    c_recv,
    b_send,
    b_recv,
):
    users, _, events = ids.shape
    inner = w_gate.shape[1]
    heads = w_dt.shape[0]
    stretches = events // STRETCH
    shares = inner // CHUNK
    part = z_states.shape[2]
    r = lax.axis_index("row")
    col = lax.axis_index("col")
    cols_axis = lax.axis_size("col")
    y, z = col // ZS, lax.rem(col, ZS)
    first = (col * ROWS + r) * events

    loads = []
    pairs = (
        (ids_in, ids),
        (table_in, table),
        (w_dt_in, w_dt),
        (bias_in, bias),
        (rates_in, rates),
        (pads_in, pads),
        (lengths_in, lengths),
        (w_in_in, w_in),
        (taps_in, taps),
        (w_gate_in, w_gate),
    )
    for i, (source, target) in enumerate(pairs):
        loads.append(pltpu.make_async_copy(source, target, load_sem.at[i]))
        loads[-1].start()

    def row_peer(d):
        return lax.rem(r + d, ROWS)

    def z_peer(d):
        return lax.rem(z + d, ZS)

    def to_row(d):
        return {"row": row_peer(d)}

    def to_z(d):
        return {"col": y * ZS + z_peer(d)}

    def to_y(d):
        return {"col": lax.rem(y + d, YS) * ZS + z}

    next_span = {
        "row": row_peer(1),
        "col": lax.rem(col + jnp.where(r == ROWS - 1, 1, 0), cols_axis),
    }
    last_span = {
        "row": row_peer(ROWS - 1),
        "col": lax.rem(col + jnp.where(r == 0, cols_axis - 1, 0), cols_axis),
    }
    barrier = pltpu.get_barrier_semaphore()
    peers = (
        [to_row(d) for d in range(1, ROWS)]
        + [to_z(d) for d in range(1, ZS)]
        + [to_y(d) for d in range(1, YS)]
        + [next_span, last_span]
    )
    for peer in peers:
        pl.semaphore_signal(barrier, inc=1, device_id=peer, device_id_type=MESH)

    sent = []

    def send(src, dst, send_sem, recv_sem, device):
        copy = pltpu.make_async_remote_copy(
            src_ref=src,
            dst_ref=dst,
            send_sem=send_sem,
            recv_sem=recv_sem,
            device_id=device,
            device_id_type=MESH,
        )
        copy.start()
        sent.append(copy)
        return copy

    lanes = lax.broadcasted_iota(jnp.int32, (STRETCH, STRETCH), 1)
    lanes_f = lanes.astype(F32)
    depths = lax.broadcasted_iota(jnp.int32, (STRETCH, STRETCH), 0)
    causal = depths >= lanes

    def one_hot(row, u, begin, rows):
        column = down_columns(row)[STRETCH - rows :, :]
        for j in range(table.shape[0] // STRETCH):
            match = column == lanes_f[:rows] + float(j * STRETCH)
            hot[u, begin : begin + rows, j * STRETCH : (j + 1) * STRETCH] = jnp.where(
                match, 1.0, 0.0
            ).astype(BF16)

    wdt_wide[...] = jnp.zeros_like(wdt_wide)
    loads[0].wait()
    for u in range(users):
        for c in range(stretches):
            row = ids[u, :, c * STRETCH : (c + 1) * STRETCH].astype(F32)
            one_hot(row, u, HALO + c * STRETCH, STRETCH)

    for load in loads[1:7]:
        load.wait()
    wdt_wide[0:heads, :] = w_dt[...]
    raw = lax.dot_general(
        table[...], wdt_wide[...], (((1,), (1,)), ((), ())), preferred_element_type=F32
    )
    raw = raw + jnp.concatenate([bias[...], jnp.zeros((1, STRETCH - heads), F32)], axis=1)
    soft = jnp.maximum(raw, 0.0) + jnp.log1p(jnp.exp(-jnp.abs(raw)))
    high = soft.astype(BF16)
    split_steps[:, 0:STRETCH] = high
    split_steps[:, STRETCH:] = (soft - high.astype(F32)).astype(BF16)
    speed = down_columns(
        jnp.concatenate([rates[...], jnp.zeros((1, STRETCH - heads), F32)], axis=1)
    )[0:heads]
    usable = {}
    for u in range(users):
        picked = dot(hot[u, HALO:, :], split_steps[...])
        step = picked[:, 0:STRETCH] + picked[:, STRETCH:]
        for c in range(stretches):
            place = first + c * STRETCH + lax.broadcasted_iota(jnp.int32, (1, STRETCH), 1)
            rows = slice(c * STRETCH, (c + 1) * STRETCH)
            kept = jnp.logical_and(place < lengths[u], pads[u, :, rows] > 0)
            usable[u, c] = jnp.where(kept, 1.0, 0.0)
            step_t = jnp.transpose(step[rows])[0:heads] * usable[u, c]
            step_rows[u, c] = step_t
            slopes[(u * stretches + c) * heads : (u * stretches + c + 1) * heads, :] = (
                step_t * speed
            )

    pl.semaphore_wait(barrier, len(peers))
    tail = slice(events - STRETCH, events)
    halo_copy = send(ids.at[:, :, tail], halo, halo_send, halo_recv, next_span)

    gained = jnp.dot(
        slopes[...],
        jnp.where(depths <= lanes, 1.0, 0.0),
        preferred_element_type=F32,
        precision=lax.Precision.HIGHEST,
    )
    for u in range(users):
        before = [jnp.zeros((heads, 1), F32)]
        log_t = []
        for c in range(stretches):
            begin = (u * stretches + c) * heads
            log_t.append(gained[begin : begin + heads])
            before.append(before[c] + log_t[c][:, STRETCH - 1 :])
        for c in range(stretches):
            rows = slice(c * STRETCH, (c + 1) * STRETCH)
            log_rows[u, c] = log_t[c]
            so_far = before[c] + log_t[c]
            to_end = jnp.exp(so_far - before[stretches]) * step_rows[u, c]
            for h in range(heads):
                tails[u, h, :, rows] = to_end[h : h + 1, :]
            columns_out[u, rows, :] = jnp.transpose(
                jnp.concatenate(
                    [
                        log_t[c],
                        jnp.broadcast_to(usable[u, c], (heads, STRETCH)),
                        jnp.exp(-so_far),
                        jnp.exp(-log_t[c]),
                        jnp.zeros((STRETCH - 4 * heads, STRETCH), F32),
                    ],
                    axis=0,
                )
            )
        for h in range(heads):
            half = h % 2
            logs[h // 2, u, :, half * STRETCH : (half + 1) * STRETCH] = jnp.broadcast_to(
                before[stretches][h : h + 1, :], (1, STRETCH)
            )
    xl_copies = [
        send(logs.at[row_peer(d)], row_logs.at[r], xl_send.at[d], xl_recv.at[d], to_row(d))
        for d in range(1, ROWS)
    ]
    row_logs[r] = logs[r]

    loads[7].wait()
    loads[8].wait()
    for j in reversed(range(shares + 1)):
        columns = slice(j * CHUNK, (j + 1) * CHUNK)
        projected[:, columns] = dot(table[...], w_in[:, columns]).astype(BF16)

    halo_copy.wait_recv()
    nobody = jnp.logical_and(r == 0, col == 0)
    for u in range(users):
        one_hot(jnp.where(nobody, -1.0, halo[u].astype(F32)), u, 0, HALO)

    joined = (joined_even, joined_odd)

    def gather(u, columns):
        rows = dot(hot[u], projected[:, columns])
        for half in range(2):
            joined[u][half] = rows[:, half * STRETCH : (half + 1) * STRETCH]

    def convolve(u, half, columns):
        total = None
        for k in range(taps.shape[0]):
            begin = HALO - taps.shape[0] + 1 + k
            term = joined[u][half, begin : begin + events, :] * taps[k : k + 1, columns]
            total = term if total is None else total + term
        return total

    for u in range(users):
        gather(u, slice(inner, inner + CHUNK))
    for u in range(users):
        into = convolve(u, 0, slice(inner, inner + STRETCH)).astype(BF16)
        inward[u] = into
        outward[u] = convolve(u, 1, slice(inner + STRETCH, inner + CHUNK)).astype(BF16)
        for c in range(stretches):
            rows = slice(c * STRETCH, (c + 1) * STRETCH)
            in_rows[u, :, rows] = jnp.transpose(into[rows].astype(F32))

    for copy in xl_copies:
        copy.wait_recv()
    block_log = row_logs[0]
    for i in range(1, ROWS):
        block_log = block_log + row_logs[i]
    z_log_out[...] = block_log
    z_logs[z] = block_log
    zl_copies = [
        send(z_log_out, z_logs.at[z], zl_send.at[d], zl_recv.at[d], to_z(d)) for d in range(1, ZS)
    ]

    x_copies = {}
    order = [(d, u) for d in (2, 1, 3, 0) for u in range(users)]

    def share(d, begin=0, size=CHUNK):
        return pl.ds(pl.multiple_of(row_peer(d) * CHUNK + begin, STRETCH), size)

    gather(order[0][1], share(order[0][0]))
    for i, (d, u) in enumerate(order):
        if i + 1 < len(order):
            gather(order[i + 1][1], share(order[i + 1][0]))
        for half in range(2):
            columns = share(d, half * STRETCH, STRETCH)
            values = silu(convolve(u, half, columns)).astype(BF16)
            signal[u, :, columns] = values
            scaled = (in_rows[u] * tails[u, 2 * row_peer(d) + half]).astype(BF16)
            state = dot(scaled, values).astype(BF16)
            cols = slice(half * STRETCH, (half + 1) * STRETCH)
            if d:
                states[u, d, :, cols] = state
            else:
                row_states[u, r, :, cols] = state
        if d:
            x_copies[u, d] = send(
                states.at[u, d],
                row_states.at[u, r],
                x_send.at[u, d],
                x_recv.at[u, d],
                to_row(d),
            )

    for copy in zl_copies:
        copy.wait_recv()
    y_log = z_logs[0]
    for i in range(1, ZS):
        y_log = y_log + z_logs[i]
    y_log_out[...] = y_log
    y_logs[y] = y_log
    yl_copies = [
        send(y_log_out, y_logs.at[y], yl_send.at[d], yl_recv.at[d], to_y(d)) for d in range(1, YS)
    ]

    loads[9].wait()

    def gate_phase(begin, end):
        @pl.loop(begin, end)
        def _(j):
            columns = pl.ds(pl.multiple_of(j * CHUNK, CHUNK), CHUNK)
            opened = dot(table[...], w_gate[:, columns]).astype(BF16)
            opened = silu(opened.astype(F32)).astype(BF16)
            for u in range(users):
                gate[u, :, columns] = dot(hot[u, HALO:, :], opened).astype(BF16)

    def local_phase(u, begin, end):
        @pl.loop(begin, end)
        def _(c):
            rows = pl.ds(pl.multiple_of(c * STRETCH, STRETCH), STRETCH)
            column = columns_out[u, rows, :]
            log_t = log_rows[u, c]
            step_t = step_rows[u, c]
            last = log_t[:, STRETCH - 1 :]
            tail_t = jnp.exp(log_t - last) * step_t
            stay = jnp.exp(-last)
            outs = outward[u, rows, :]
            in_t = in_rows[u, :, rows]
            scores = dot(outs, in_t.astype(BF16))
            for h in range(heads):
                cols = slice(h * STRETCH, (h + 1) * STRETCH)
                gap = jnp.where(causal, log_t[h : h + 1, :] - column[:, h : h + 1], -1e30)
                weights = (scores * jnp.exp(gap) * step_t[h : h + 1, :]).astype(BF16)
                values = signal[u, rows, cols]
                entering = jnp.where(c == 0, 0.0, running[:, cols])
                fade = column[:, 3 * heads + h : 3 * heads + h + 1]
                mix[u, rows, cols] = (
                    dot(weights, values) + dot(outs, entering.astype(BF16)) * fade
                ).astype(BF16)
                scaled = (in_t * tail_t[h : h + 1, :]).astype(BF16)
                running[:, cols] = stay[h : h + 1, :] * entering + dot(scaled, values)

    gate_phase(0, shares // 2)

    for u in range(users):
        for d in range(1, ROWS):
            x_copies[u, d].wait_recv()
        total = row_states[u, 0].astype(F32)
        for i in range(1, ROWS):
            row_before[u, i - 1] = total
            total = jnp.exp(-row_logs[i, u]) * total + row_states[u, i].astype(F32)
        block = total.astype(BF16)
        for k in range(ZS):
            z_out[k, u] = block[k * part : (k + 1) * part]
    z_states[z] = z_out[z]
    z_copies = [
        send(z_out.at[z_peer(d)], z_states.at[z], z_send.at[d], z_recv.at[d], to_z(d))
        for d in (4, 3, 5, 2, 6, 1, 7)
    ]

    gate_phase(shares // 2, shares)
    local_phase(0, 0, 2)

    for copy in z_copies:
        copy.wait_recv()
    total = z_states[0].astype(F32)
    for i in range(1, ZS):
        z_before[i - 1] = total
        total = jnp.exp(-z_logs[i]) * total + z_states[i].astype(F32)
    y_out[...] = total.astype(BF16)
    y_copies = [
        send(y_out, y_states.at[y], y_send.at[d], y_recv.at[d], to_y(d)) for d in (2, 1, 3)
    ]

    local_phase(0, 2, stretches)

    for copy in yl_copies:
        copy.wait_recv()
    for copy in y_copies:
        copy.wait_recv()
    entering = jnp.zeros(y_out.shape, F32)
    for i in range(YS - 1):
        entering = jnp.where(
            i < y, jnp.exp(-y_logs[i]) * entering + y_states[i].astype(F32), entering
        )
    gone = None
    for k in range(ZS):
        value = entering
        if k:
            gone = z_logs[k - 1] if gone is None else gone + z_logs[k - 1]
            value = jnp.exp(-gone) * entering + z_before[k - 1]
        c_out[k] = value.astype(BF16)
    c_states[z] = c_out[z]
    c_copies = [
        send(c_out.at[z_peer(d)], c_states.at[z], c_send.at[d], c_recv.at[d], to_z(d))
        for d in (4, 3, 5, 2, 6, 1, 7)
    ]

    local_phase(1, 0, stretches)

    for copy in c_copies:
        copy.wait_recv()
    gone = [None, row_logs[0]]
    for i in range(2, ROWS):
        gone.append(gone[-1] + row_logs[i - 1])
    for u in range(users):
        for i in range(ROWS):
            for k in range(ZS):
                rows = slice(k * part, (k + 1) * part)
                value = c_states[k, u].astype(F32)
                if i:
                    value = jnp.exp(-gone[i][u]) * value + row_before[u, i - 1, rows, :]
                back_out[u, i, rows, :] = value.astype(BF16)
        carry[u, r] = back_out[u, r]
        for d in (2, 1, 3):
            x_copies[u, -d] = send(
                back_out.at[u, row_peer(d)],
                carry.at[u, r],
                b_send.at[u, d],
                b_recv.at[u, d],
                to_row(d),
            )
    for u in range(users):
        for d in range(1, ROWS):
            x_copies[u, -d].wait_recv()
    for copy in sent:
        copy.wait_send()


def final_kernel(carry, mix, gate, outward, columns_in, gain, w_out, result, gated, normed, done, sems):
    users, events, inner = mix.shape
    heads = inner // STRETCH
    width = w_out.shape[1]

    def norm(u, c):
        rows = slice(c * STRETCH, (c + 1) * STRETCH)
        outs = outward[u, rows, :]
        squares = jnp.zeros((STRETCH, STRETCH), F32)
        for r in range(ROWS):
            carried = dot(outs, carry[u, r])
            for half in range(2):
                h = 2 * r + half
                cols = slice(h * STRETCH, (h + 1) * STRETCH)
                fade = columns_in[u, rows, 2 * heads + h : 2 * heads + h + 1]
                value = fade * carried[:, half * STRETCH : (half + 1) * STRETCH]
                value = value + mix[u, rows, cols].astype(F32)
                value = value * gate[u, rows, cols].astype(F32)
                squares = squares + value * value
                gated[c % 2, :, cols] = value
        mean = jnp.sum(squares, axis=1, keepdims=True) * (1.0 / inner)
        scale = lax.rsqrt(mean + 1.0)
        for h in range(heads):
            cols = slice(h * STRETCH, (h + 1) * STRETCH)
            normed[u, rows, cols] = (gated[c % 2, :, cols] * scale * gain[:, cols]).astype(BF16)

    copies = []

    def project(u, j):
        columns = slice(j * CHUNK, (j + 1) * CHUNK)
        usable = columns_in[u, :, heads : heads + 1]
        done[u, :, columns] = (dot(normed[u], w_out[:, columns]) * usable).astype(BF16)
        return columns

    def store(u, j, columns):
        copy = pltpu.make_async_copy(
            done.at[u, :, columns], result.at[u, 0, :, columns], sems.at[u, j]
        )
        copy.start()
        copies.append(copy)

    blocks = events // STRETCH
    for c in range(blocks):
        norm(0, c)
    for u in range(users):
        for j in range(width // CHUNK):
            columns = project(u, j)
            if u + 1 < users and j < blocks:
                norm(u + 1, j)
            store(u, j, columns)
    for copy in copies:
        copy.wait()


def per_device(
    item_ids,
    pad_masks,
    lengths,
    item_table,
    w_gate,
    w_in,
    w_dt,
    conv_taps,
    dt_bias,
    decay_rates,
    norm_gain,
    w_out,
):
    users, _, events = item_ids.shape
    items, width = item_table.shape
    inner = w_gate.shape[1]
    full = w_in.shape[1]
    heads = decay_rates.shape[0]
    stretches = events // STRETCH
    pair = 2 * STRETCH
    part = STRETCH // ZS
    vmem = pl.BlockSpec(memory_space=pltpu.VMEM)
    hbm = pl.BlockSpec(memory_space=pltpu.HBM)
    dma = pltpu.SemaphoreType.DMA
    carry, mix, gate, outward, decays = pl.pallas_call(
        main_kernel,
        name="main",
        out_shape=(
            jax.ShapeDtypeStruct((users, ROWS, STRETCH, pair), BF16),
            jax.ShapeDtypeStruct((users, events, inner), BF16),
            jax.ShapeDtypeStruct((users, events, inner), BF16),
            jax.ShapeDtypeStruct((users, events, STRETCH), BF16),
            jax.ShapeDtypeStruct((users, events, STRETCH), F32),
        ),
        in_specs=[hbm] * 10,
        out_specs=(vmem,) * 5,
        scratch_shapes=[
            pltpu.SMEM(lengths.shape, lengths.dtype),
            pltpu.VMEM(item_ids.shape, item_ids.dtype),
            pltpu.VMEM(pad_masks.shape, pad_masks.dtype),
            pltpu.VMEM((heads, width), BF16),
            pltpu.VMEM(conv_taps.shape, F32),
            pltpu.VMEM((1, heads), F32),
            pltpu.VMEM((1, heads), F32),
            pltpu.VMEM((items, width), BF16),
            pltpu.VMEM((width, full), BF16),
            pltpu.VMEM((width, inner), BF16),
            pltpu.VMEM((STRETCH, width), BF16),
            pltpu.VMEM((items, 2 * STRETCH), BF16),
            pltpu.VMEM((users, 1, STRETCH), jnp.int32),
            pltpu.VMEM((users, HALO + events, items), BF16),
            pltpu.VMEM((items, full), BF16),
            pltpu.VMEM((2, HALO + events, STRETCH), F32),
            pltpu.VMEM((2, HALO + events, STRETCH), F32),
            pltpu.VMEM((users, events, inner), BF16),
            pltpu.VMEM((users, events, STRETCH), BF16),
            pltpu.VMEM((users, STRETCH, events), F32),
            pltpu.VMEM((users * stretches * heads, STRETCH), F32),
            pltpu.VMEM((users, stretches, heads, STRETCH), F32),
            pltpu.VMEM((users, stretches, heads, STRETCH), F32),
            pltpu.VMEM((users, heads, 1, events), F32),
            pltpu.VMEM((STRETCH, inner), F32),
            pltpu.VMEM((users, ROWS, STRETCH, pair), BF16),
            pltpu.VMEM((ROWS, users, 1, pair), F32),
            pltpu.VMEM((users, ROWS, STRETCH, pair), BF16),
            pltpu.VMEM((ROWS, users, 1, pair), F32),
            pltpu.VMEM((users, ROWS - 1, STRETCH, pair), F32),
            pltpu.VMEM((ZS, users, part, pair), BF16),
            pltpu.VMEM((ZS, users, part, pair), BF16),
            pltpu.VMEM((ZS - 1, users, part, pair), F32),
            pltpu.VMEM((users, 1, pair), F32),
            pltpu.VMEM((ZS, users, 1, pair), F32),
            pltpu.VMEM((users, part, pair), BF16),
            pltpu.VMEM((YS, users, part, pair), BF16),
            pltpu.VMEM((users, 1, pair), F32),
            pltpu.VMEM((YS, users, 1, pair), F32),
            pltpu.VMEM((ZS, users, part, pair), BF16),
            pltpu.VMEM((ZS, users, part, pair), BF16),
            pltpu.VMEM((users, ROWS, STRETCH, pair), BF16),
            dma((10,)),
            dma,
            dma,
        ]
        + [dma((users, ROWS))] * 2
        + [dma((ROWS,))] * 2
        + [dma((ZS,))] * 4
        + [dma((YS,))] * 4
        + [dma((ZS,))] * 2
        + [dma((users, ROWS))] * 2,
        compiler_params=pltpu.CompilerParams(
            collective_id=0, has_side_effects=True, vmem_limit_bytes=36 << 20
        ),
    )(
        *(
            pltpu.with_memory_space_constraint(array, pltpu.HBM)
            for array in (
                lengths,
                item_ids,
                pad_masks,
                w_dt.T,
                conv_taps,
                dt_bias.reshape(1, heads),
                decay_rates.reshape(1, heads),
                item_table,
                w_in,
                w_gate,
            )
        )
    )
    return pl.pallas_call(
        final_kernel,
        name="final",
        out_shape=jax.ShapeDtypeStruct((users, 1, events, w_out.shape[1]), BF16),
        in_specs=[vmem] * 7,
        out_specs=hbm,
        scratch_shapes=[
            pltpu.VMEM((2, STRETCH, inner), F32),
            pltpu.VMEM((users, events, inner), BF16),
            pltpu.VMEM((users, events, w_out.shape[1]), BF16),
            dma((users, w_out.shape[1] // CHUNK)),
        ],
        compiler_params=pltpu.CompilerParams(vmem_limit_bytes=24 << 20),
    )(carry, mix, gate, outward, decays, norm_gain.reshape(1, inner), w_out)


def solution(mesh):
    spans = P("batch", "col", "row")
    return jax.shard_map(
        per_device,
        mesh=mesh,
        in_specs=(spans, spans, P("batch")) + (P(),) * 9,
        out_specs=P("batch", "col", "row", None),
        check_vma=False,
    )
```

```python
import jax
import jax.numpy as jnp
from jax import lax
from jax.experimental import pallas as pl
from jax.experimental.pallas import tpu as pltpu
from jax.sharding import PartitionSpec as P

STRETCH = 128
CHUNK = 256
HALO = 16
ROWS, YS, ZS = 4, 4, 8
MESH = pl.DeviceIdType.MESH
BF16 = jnp.bfloat16
F32 = jnp.float32


def silu_of_half(v):
    return v + v * jnp.tanh(v)


def dot(a, b):
    return jnp.dot(a, b, preferred_element_type=F32)


def down_columns(row):
    return jnp.transpose(jnp.broadcast_to(row, (STRETCH, STRETCH)))


def main_kernel(
    lengths_in,
    ids_in,
    pads_in,
    w_dt_in,
    taps_in,
    bias_in,
    rates_in,
    table_in,
    w_in_in,
    w_gate_in,
    w_out_in,
    gain_in,
    carry,
    mix,
    gate,
    outward,
    columns_out,
    total_out,
    squares,
    lengths,
    ids,
    pads,
    w_dt,
    taps,
    bias,
    rates,
    table,
    w_in,
    w_gate,
    w_out,
    gain,
    half_taps,
    turned,
    gated,
    wdt_wide,
    split_steps,
    halo,
    hot,
    projected,
    joined_even,
    joined_odd,
    signal,
    in_rows,
    slopes,
    log_rows,
    step_rows,
    tails,
    running,
    states,
    logs,
    row_states,
    row_logs,
    row_before,
    z_out,
    z_states,
    z_before,
    z_log_out,
    z_logs,
    y_out,
    y_states,
    y_log_out,
    y_logs,
    c_out,
    c_states,
    back_out,
    load_sem,
    near,
    halo_send,
    halo_recv,
    x_send,
    x_recv,
    xl_send,
    xl_recv,
    z_send,
    z_recv,
    zl_send,
    zl_recv,
    y_send,
    y_recv,
    yl_send,
    yl_recv,
    c_send,
    c_recv,
    b_send,
    b_recv,
):
    users, _, events = ids.shape
    inner = w_gate.shape[1]
    heads = w_dt.shape[0]
    stretches = events // STRETCH
    shares = inner // CHUNK
    part = z_states.shape[2]
    r = lax.axis_index("row")
    col = lax.axis_index("col")
    cols_axis = lax.axis_size("col")
    y, z = col // ZS, lax.rem(col, ZS)
    first = (col * ROWS + r) * events

    def row_peer(d):
        return lax.rem(r + d, ROWS)

    def share(d, begin=0, size=CHUNK):
        return pl.ds(pl.multiple_of(row_peer(d) * CHUNK + begin, STRETCH), size)

    shares_order = (2, 1, 3, 0)
    maps = slice(inner, inner + CHUNK)
    loads = []
    pairs = [
        (ids_in, ids),
        (table_in, table),
        (w_dt_in, w_dt),
        (bias_in, bias),
        (rates_in, rates),
        (pads_in, pads),
        (lengths_in, lengths),
        (w_in_in.at[:, maps], w_in.at[:, maps]),
        (taps_in, taps),
    ]
    pairs += [(w_in_in.at[:, share(d)], w_in.at[:, share(d)]) for d in shares_order]
    pairs += [(w_gate_in, w_gate), (w_out_in, w_out), (gain_in, gain)]
    for i, (source, target) in enumerate(pairs):
        loads.append(pltpu.make_async_copy(source, target, load_sem.at[i]))
        loads[-1].start()

    def z_peer(d):
        return lax.rem(z + d, ZS)

    def to_row(d):
        return {"row": row_peer(d)}

    def to_z(d):
        return {"col": y * ZS + z_peer(d)}

    def to_y(d):
        return {"col": lax.rem(y + d, YS) * ZS + z}

    next_span = {
        "row": row_peer(1),
        "col": lax.rem(col + jnp.where(r == ROWS - 1, 1, 0), cols_axis),
    }
    last_span = {
        "row": row_peer(ROWS - 1),
        "col": lax.rem(col + jnp.where(r == 0, cols_axis - 1, 0), cols_axis),
    }
    barrier = pltpu.get_barrier_semaphore()
    peers = (
        [to_row(d) for d in range(1, ROWS)]
        + [next_span, last_span]
        + [to_z(1), to_z(ZS - 1), to_y(1), to_y(YS - 1)]
    )
    for peer in peers:
        pl.semaphore_signal(barrier, inc=1, device_id=peer, device_id_type=MESH)

    def tell(index, devices):
        for device in devices:
            pl.semaphore_signal(near.at[index], inc=1, device_id=device, device_id_type=MESH)

    sides = [to_z(1), to_z(ZS - 1)]
    sent = []

    def send(src, dst, send_sem, recv_sem, device):
        copy = pltpu.make_async_remote_copy(
            src_ref=src,
            dst_ref=dst,
            send_sem=send_sem,
            recv_sem=recv_sem,
            device_id=device,
            device_id_type=MESH,
        )
        copy.start()
        sent.append(copy)
        return copy

    lanes = lax.broadcasted_iota(jnp.int32, (STRETCH, STRETCH), 1)
    lanes_f = lanes.astype(F32)
    depths = lax.broadcasted_iota(jnp.int32, (STRETCH, STRETCH), 0)
    causal = depths >= lanes

    def one_hot(row, u, begin, rows):
        column = down_columns(row)[STRETCH - rows :, :]
        for j in range(table.shape[0] // STRETCH):
            match = column == lanes_f[:rows] + float(j * STRETCH)
            hot[u, begin : begin + rows, j * STRETCH : (j + 1) * STRETCH] = jnp.where(
                match, 1.0, 0.0
            ).astype(BF16)

    wdt_wide[...] = jnp.zeros_like(wdt_wide)
    loads[0].wait()
    for u in range(users):
        for c in range(stretches):
            row = ids[u, :, c * STRETCH : (c + 1) * STRETCH].astype(F32)
            one_hot(row, u, HALO + c * STRETCH, STRETCH)

    for load in loads[1:7]:
        load.wait()
    wdt_wide[0:heads, :] = w_dt[...]
    raw = lax.dot_general(
        table[...], wdt_wide[...], (((1,), (1,)), ((), ())), preferred_element_type=F32
    )
    raw = raw + jnp.concatenate([bias[...], jnp.zeros((1, STRETCH - heads), F32)], axis=1)
    soft = jnp.maximum(raw, 0.0) + jnp.log1p(jnp.exp(-jnp.abs(raw)))
    high = soft.astype(BF16)
    split_steps[:, 0:STRETCH] = high
    split_steps[:, STRETCH:] = (soft - high.astype(F32)).astype(BF16)
    pl.semaphore_wait(barrier, len(peers))
    tail = slice(events - STRETCH, events)
    halo_copy = send(ids.at[:, :, tail], halo, halo_send, halo_recv, next_span)
    tell(0, sides)
    tell(3, [to_y(1), to_y(YS - 1)])
    speed = down_columns(
        jnp.concatenate([rates[...], jnp.zeros((1, STRETCH - heads), F32)], axis=1)
    )[0:heads]
    usable = {}
    for u in range(users):
        picked = dot(hot[u, HALO:, :], split_steps[...])
        step = picked[:, 0:STRETCH] + picked[:, STRETCH:]
        for c in range(stretches):
            place = first + c * STRETCH + lax.broadcasted_iota(jnp.int32, (1, STRETCH), 1)
            rows = slice(c * STRETCH, (c + 1) * STRETCH)
            kept = jnp.logical_and(place < lengths[u], pads[u, :, rows] > 0)
            usable[u, c] = jnp.where(kept, 1.0, 0.0)
            step_t = jnp.transpose(step[rows])[0:heads] * usable[u, c]
            step_rows[u, c] = step_t
            slopes[(u * stretches + c) * heads : (u * stretches + c + 1) * heads, :] = (
                step_t * speed
            )

    gained = jnp.dot(
        slopes[...],
        jnp.where(depths <= lanes, 1.0, 0.0),
        preferred_element_type=F32,
        precision=lax.Precision.HIGHEST,
    )
    for u in range(users):
        before = [jnp.zeros((heads, 1), F32)]
        log_t = []
        for c in range(stretches):
            begin = (u * stretches + c) * heads
            log_t.append(gained[begin : begin + heads])
            before.append(before[c] + log_t[c][:, STRETCH - 1 :])
        for c in range(stretches):
            rows = slice(c * STRETCH, (c + 1) * STRETCH)
            log_rows[u, c] = log_t[c]
            so_far = before[c] + log_t[c]
            to_end = jnp.exp(so_far - before[stretches]) * step_rows[u, c]
            for h in range(heads):
                tails[u, h, :, rows] = to_end[h : h + 1, :]
            left = jnp.exp(-so_far)
            turned[u, c, 0:heads, :] = left
            turned[u, c, heads:, :] = left
            columns_out[u, rows, :] = jnp.transpose(
                jnp.concatenate(
                    [
                        log_t[c],
                        jnp.broadcast_to(usable[u, c], (heads, STRETCH)),
                        turned[u, c, pl.ds(2 * r, heads), :],
                        jnp.exp(-log_t[c]),
                        jnp.zeros((STRETCH - 4 * heads, STRETCH), F32),
                    ],
                    axis=0,
                )
            )
        for h in range(heads):
            half = h % 2
            logs[h // 2, u, :, half * STRETCH : (half + 1) * STRETCH] = jnp.broadcast_to(
                before[stretches][h : h + 1, :], (1, STRETCH)
            )
    pl.semaphore_wait(near.at[0], 2)
    tell(1, sides)
    xl_copies = [
        send(logs.at[row_peer(d)], row_logs.at[r], xl_send.at[d], xl_recv.at[d], to_row(d))
        for d in range(1, ROWS)
    ]
    row_logs[r] = logs[r]

    loads[7].wait()
    loads[8].wait()
    half_taps[...] = 0.5 * taps[...]

    def project(slot, columns):
        projected[slot] = dot(table[...], w_in[:, columns]).astype(BF16)

    project(ROWS, maps)
    loads[9].wait()
    project(2, share(2))
    pl.semaphore_wait(near.at[1], 2)
    tell(2, sides)

    halo_copy.wait_recv()
    nobody = jnp.logical_and(r == 0, col == 0)
    for u in range(users):
        one_hot(jnp.where(nobody, -1.0, halo[u].astype(F32)), u, 0, HALO)

    joined = (joined_even, joined_odd)

    def gather(u, slot):
        rows = dot(hot[u], projected[slot])
        for half in range(2):
            joined[u][half] = rows[:, half * STRETCH : (half + 1) * STRETCH]

    def convolve(u, half, weights, columns):
        total = None
        for k in range(weights.shape[0]):
            begin = HALO - weights.shape[0] + 1 + k
            term = joined[u][half, begin : begin + events, :] * weights[k : k + 1, columns]
            total = term if total is None else total + term
        return total

    for u in range(users):
        gather(u, ROWS)
    for u in range(users):
        into = convolve(u, 0, taps, slice(inner, inner + STRETCH)).astype(BF16)
        outs = convolve(u, 1, taps, slice(inner + STRETCH, inner + CHUNK))
        outward[u] = outs.astype(BF16)
        for c in range(stretches):
            rows = slice(c * STRETCH, (c + 1) * STRETCH)
            in_rows[u, :, rows] = jnp.transpose(into[rows].astype(F32))

    x_copies = {}
    order = [(d, u) for d in shares_order for u in range(users)]

    def state_step(i):
        d, u = order[i]
        if i + 1 < len(order):
            gather(order[i + 1][1], order[i + 1][0])
        for half in range(2):
            columns = share(d, half * STRETCH, STRETCH)
            values = silu_of_half(convolve(u, half, half_taps, columns)).astype(BF16)
            signal[u, :, columns] = values
            scaled = (in_rows[u] * tails[u, 2 * row_peer(d) + half]).astype(BF16)
            state = dot(scaled, values).astype(BF16)
            cols = slice(half * STRETCH, (half + 1) * STRETCH)
            if d:
                states[u, d, :, cols] = state
            else:
                row_states[u, r, :, cols] = state
        if d:
            x_copies[u, d] = send(
                states.at[u, d],
                row_states.at[u, r],
                x_send.at[u, d],
                x_recv.at[u, d],
                to_row(d),
            )

    gather(order[0][1], 2)
    state_step(0)
    for load in loads[10:13]:
        load.wait()
    project(1, share(1))
    state_step(1)
    project(3, share(3))
    state_step(2)

    for copy in xl_copies:
        copy.wait_recv()
    block_log = row_logs[0]
    for i in range(1, ROWS):
        block_log = block_log + row_logs[i]
    z_log_out[...] = block_log
    z_logs[z] = block_log
    pl.semaphore_wait(near.at[2], 2)
    pl.semaphore_wait(near.at[3], 2)
    zl_copies = [
        send(z_log_out, z_logs.at[z], zl_send.at[d], zl_recv.at[d], to_z(d)) for d in range(1, ZS)
    ]

    project(0, share(0))
    for i in range(3, len(order)):
        state_step(i)

    for copy in zl_copies:
        copy.wait_recv()
    y_log = z_logs[0]
    for i in range(1, ZS):
        y_log = y_log + z_logs[i]
    y_log_out[...] = y_log
    y_logs[y] = y_log
    yl_copies = [
        send(y_log_out, y_logs.at[y], yl_send.at[d], yl_recv.at[d], to_y(d)) for d in range(1, YS)
    ]

    loads[13].wait()

    def gate_phase(begin, end):
        @pl.loop(begin, end)
        def _(j):
            columns = pl.ds(pl.multiple_of(j * CHUNK, CHUNK), CHUNK)
            opened = dot(table[...], w_gate[:, columns]).astype(BF16)
            opened = silu_of_half(0.5 * opened.astype(F32)).astype(BF16)
            for u in range(users):
                gate[u, :, columns] = dot(hot[u, HALO:, :], opened).astype(BF16)

    def local_phase(u, begin, end):
        @pl.loop(begin, end)
        def _(c):
            rows = pl.ds(pl.multiple_of(c * STRETCH, STRETCH), STRETCH)
            column = columns_out[u, rows, :]
            log_t = log_rows[u, c]
            step_t = step_rows[u, c]
            last = log_t[:, STRETCH - 1 :]
            tail_t = jnp.exp(log_t - last) * step_t
            stay = jnp.exp(-last)
            outs = outward[u, rows, :]
            in_t = in_rows[u, :, rows]
            scores = dot(outs, in_t.astype(BF16))
            for h in range(heads):
                cols = slice(h * STRETCH, (h + 1) * STRETCH)
                gap = jnp.where(causal, log_t[h : h + 1, :] - column[:, h : h + 1], -1e30)
                weights = (scores * jnp.exp(gap) * step_t[h : h + 1, :]).astype(BF16)
                values = signal[u, rows, cols]
                entering = jnp.where(c == 0, 0.0, running[:, cols])
                fade = column[:, 3 * heads + h : 3 * heads + h + 1]
                mix[u, rows, cols] = (
                    dot(weights, values) + dot(outs, entering.astype(BF16)) * fade
                ).astype(BF16)
                scaled = (in_t * tail_t[h : h + 1, :]).astype(BF16)
                running[:, cols] = stay[h : h + 1, :] * entering + dot(scaled, values)

    gate_phase(0, shares // 2)

    for u in range(users):
        for d in range(1, ROWS):
            x_copies[u, d].wait_recv()
        total = row_states[u, 0].astype(F32)
        for i in range(1, ROWS):
            row_before[u, i - 1] = total
            total = jnp.exp(-row_logs[i, u]) * total + row_states[u, i].astype(F32)
        block = total.astype(BF16)
        for k in range(ZS):
            z_out[k, u] = block[k * part : (k + 1) * part]
    z_states[z] = z_out[z]
    z_copies = [
        send(z_out.at[z_peer(d)], z_states.at[z], z_send.at[d], z_recv.at[d], to_z(d))
        for d in (4, 3, 5, 2, 6, 1, 7)
    ]

    gate_phase(shares // 2, shares)
    local_phase(0, 0, 2)

    for copy in z_copies:
        copy.wait_recv()
    total = z_states[0].astype(F32)
    for i in range(1, ZS):
        z_before[i - 1] = total
        total = jnp.exp(-z_logs[i]) * total + z_states[i].astype(F32)
    y_out[...] = total.astype(BF16)
    y_copies = [
        send(y_out, y_states.at[y], y_send.at[d], y_recv.at[d], to_y(d)) for d in (2, 1, 3)
    ]

    local_phase(0, 2, stretches)

    for copy in yl_copies:
        copy.wait_recv()
    for copy in y_copies:
        copy.wait_recv()
    entering = jnp.zeros(y_out.shape, F32)
    for i in range(YS - 1):
        entering = jnp.where(
            i < y, jnp.exp(-y_logs[i]) * entering + y_states[i].astype(F32), entering
        )
    gone = None
    for k in range(ZS):
        value = entering
        if k:
            gone = z_logs[k - 1] if gone is None else gone + z_logs[k - 1]
            value = jnp.exp(-gone) * entering + z_before[k - 1]
        c_out[k] = value.astype(BF16)
    c_states[z] = c_out[z]
    c_copies = [
        send(c_out.at[z_peer(d)], c_states.at[z], c_send.at[d], c_recv.at[d], to_z(d))
        for d in (4, 3, 5, 2, 6, 1, 7)
    ]

    local_phase(1, 0, stretches)

    for copy in c_copies:
        copy.wait_recv()
    gone = [None, row_logs[0]]
    for i in range(2, ROWS):
        gone.append(gone[-1] + row_logs[i - 1])
    for u in range(users):
        for i in range(ROWS):
            for k in range(ZS):
                rows = slice(k * part, (k + 1) * part)
                value = c_states[k, u].astype(F32)
                if i:
                    value = jnp.exp(-gone[i][u]) * value + row_before[u, i - 1, rows, :]
                back_out[u, i, rows, :] = value.astype(BF16)
        carry[u, r] = back_out[u, r]
        for d in (2, 1, 3):
            x_copies[u, -d] = send(
                back_out.at[u, row_peer(d)],
                carry.at[u, r],
                b_send.at[u, d],
                b_recv.at[u, d],
                to_row(d),
            )
    for load in loads[14:]:
        load.wait()

    def share_step(u, d):
        for c in range(stretches):
            rows = slice(c * STRETCH, (c + 1) * STRETCH)
            carried = dot(outward[u, rows, :], carry[u, row_peer(d)])
            both = None
            for half in range(2):
                cols = share(d, half * STRETCH, STRETCH)
                place = 2 * heads + 2 * d + half
                value = (
                    columns_out[u, rows, place : place + 1]
                    * carried[:, half * STRETCH : (half + 1) * STRETCH]
                    + mix[u, rows, cols].astype(F32)
                ) * gate[u, rows, cols].astype(F32)
                gated[rows, half * STRETCH : (half + 1) * STRETCH] = (
                    value * gain[:, cols]
                ).astype(BF16)
                both = value * value if both is None else both + value * value
            squares[u, rows, :] = squares[u, rows, :] + both if d else both
        for j in range(w_out.shape[1] // CHUNK):
            columns = slice(j * CHUNK, (j + 1) * CHUNK)
            term = dot(gated[...], w_out[share(d), columns])
            total_out[u, :, columns] = total_out[u, :, columns] + term if d else term

    for u in range(users):
        share_step(u, 0)
    for u in range(users):
        for d in (1, 3) if u + 1 == users else (1, 3, 2):
            x_copies[u, -d].wait_recv()
            share_step(u, ROWS - d)
    x_copies[users - 1, -2].wait_recv()
    for copy in sent:
        copy.wait_send()


def final_kernel(
    carry, mix, gate, outward, columns_in, totals, squares, gain, w_out, result, gated, done, sems
):
    users, events, inner = mix.shape
    heads = inner // STRETCH
    width = w_out.shape[1]
    last = users - 1
    owner = lax.rem(lax.axis_index("row") + 2, ROWS)
    copies = []
    scale = {}

    def scale_of(u, more):
        total = squares[u] if more is None else squares[u] + more
        mean = jnp.sum(total, axis=1, keepdims=True) * (1.0 / inner)
        return lax.rsqrt(mean + 1.0) * columns_in[u, :, heads : heads + 1]

    def store(u, j, values):
        columns = slice(j * CHUNK, (j + 1) * CHUNK)
        done[u, :, columns] = (values * scale[u]).astype(BF16)
        copy = pltpu.make_async_copy(
            done.at[u, :, columns], result.at[u, 0, :, columns], sems.at[u, j]
        )
        copy.start()
        copies.append(copy)

    both = []
    for c in range(events // STRETCH):
        rows = slice(c * STRETCH, (c + 1) * STRETCH)
        carried = dot(outward[last, rows, :], carry[last, owner])
        added = None
        for half in range(2):
            cols = pl.ds(pl.multiple_of(owner * CHUNK + half * STRETCH, STRETCH), STRETCH)
            place = 2 * heads + 2 * 2 + half
            value = (
                columns_in[last, rows, place : place + 1]
                * carried[:, half * STRETCH : (half + 1) * STRETCH]
                + mix[last, rows, cols].astype(F32)
            ) * gate[last, rows, cols].astype(F32)
            gated[rows, half * STRETCH : (half + 1) * STRETCH] = (value * gain[:, cols]).astype(
                BF16
            )
            added = value * value if added is None else added + value * value
        both.append(added)
    for u in range(users):
        scale[u] = scale_of(u, jnp.concatenate(both, axis=0) if u == last else None)
    for u in range(users):
        for j in range(width // CHUNK):
            columns = slice(j * CHUNK, (j + 1) * CHUNK)
            values = totals[u, :, columns]
            if u == last:
                rows = pl.ds(pl.multiple_of(owner * CHUNK, CHUNK), CHUNK)
                values = values + dot(gated[...], w_out[rows, columns])
            store(u, j, values)
    for copy in copies:
        copy.wait()


def per_device(
    item_ids,
    pad_masks,
    lengths,
    item_table,
    w_gate,
    w_in,
    w_dt,
    conv_taps,
    dt_bias,
    decay_rates,
    norm_gain,
    w_out,
):
    users, _, events = item_ids.shape
    items, width = item_table.shape
    inner = w_gate.shape[1]
    full = w_in.shape[1]
    heads = decay_rates.shape[0]
    stretches = events // STRETCH
    pair = 2 * STRETCH
    part = STRETCH // ZS
    vmem = pl.BlockSpec(memory_space=pltpu.VMEM)
    hbm = pl.BlockSpec(memory_space=pltpu.HBM)
    dma = pltpu.SemaphoreType.DMA
    carry, mix, gate, outward, columns, totals, squares = pl.pallas_call(
        main_kernel,
        name="main",
        out_shape=(
            jax.ShapeDtypeStruct((users, ROWS, STRETCH, pair), BF16),
            jax.ShapeDtypeStruct((users, events, inner), BF16),
            jax.ShapeDtypeStruct((users, events, inner), BF16),
            jax.ShapeDtypeStruct((users, events, STRETCH), BF16),
            jax.ShapeDtypeStruct((users, events, STRETCH), F32),
            jax.ShapeDtypeStruct((users, events, w_out.shape[1]), F32),
            jax.ShapeDtypeStruct((users, events, STRETCH), F32),
        ),
        in_specs=[hbm] * 12,
        out_specs=(vmem,) * 7,
        scratch_shapes=[
            pltpu.SMEM(lengths.shape, lengths.dtype),
            pltpu.VMEM(item_ids.shape, item_ids.dtype),
            pltpu.VMEM(pad_masks.shape, pad_masks.dtype),
            pltpu.VMEM((heads, width), BF16),
            pltpu.VMEM(conv_taps.shape, F32),
            pltpu.VMEM((1, heads), F32),
            pltpu.VMEM((1, heads), F32),
            pltpu.VMEM((items, width), BF16),
            pltpu.VMEM((width, full), BF16),
            pltpu.VMEM((width, inner), BF16),
            pltpu.VMEM(w_out.shape, BF16),
            pltpu.VMEM((1, inner), F32),
            pltpu.VMEM(conv_taps.shape, F32),
            pltpu.VMEM((users, stretches, 2 * heads, STRETCH), F32),
            pltpu.VMEM((events, CHUNK), BF16),
            pltpu.VMEM((STRETCH, width), BF16),
            pltpu.VMEM((items, 2 * STRETCH), BF16),
            pltpu.VMEM((users, 1, STRETCH), jnp.int32),
            pltpu.VMEM((users, HALO + events, items), BF16),
            pltpu.VMEM((ROWS + 1, items, CHUNK), BF16),
            pltpu.VMEM((2, HALO + events, STRETCH), F32),
            pltpu.VMEM((2, HALO + events, STRETCH), F32),
            pltpu.VMEM((users, events, inner), BF16),
            pltpu.VMEM((users, STRETCH, events), F32),
            pltpu.VMEM((users * stretches * heads, STRETCH), F32),
            pltpu.VMEM((users, stretches, heads, STRETCH), F32),
            pltpu.VMEM((users, stretches, heads, STRETCH), F32),
            pltpu.VMEM((users, heads, 1, events), F32),
            pltpu.VMEM((STRETCH, inner), F32),
            pltpu.VMEM((users, ROWS, STRETCH, pair), BF16),
            pltpu.VMEM((ROWS, users, 1, pair), F32),
            pltpu.VMEM((users, ROWS, STRETCH, pair), BF16),
            pltpu.VMEM((ROWS, users, 1, pair), F32),
            pltpu.VMEM((users, ROWS - 1, STRETCH, pair), F32),
            pltpu.VMEM((ZS, users, part, pair), BF16),
            pltpu.VMEM((ZS, users, part, pair), BF16),
            pltpu.VMEM((ZS - 1, users, part, pair), F32),
            pltpu.VMEM((users, 1, pair), F32),
            pltpu.VMEM((ZS, users, 1, pair), F32),
            pltpu.VMEM((users, part, pair), BF16),
            pltpu.VMEM((YS, users, part, pair), BF16),
            pltpu.VMEM((users, 1, pair), F32),
            pltpu.VMEM((YS, users, 1, pair), F32),
            pltpu.VMEM((ZS, users, part, pair), BF16),
            pltpu.VMEM((ZS, users, part, pair), BF16),
            pltpu.VMEM((users, ROWS, STRETCH, pair), BF16),
            dma((16,)),
            pltpu.SemaphoreType.REGULAR((4,)),
            dma,
            dma,
        ]
        + [dma((users, ROWS))] * 2
        + [dma((ROWS,))] * 2
        + [dma((ZS,))] * 4
        + [dma((YS,))] * 4
        + [dma((ZS,))] * 2
        + [dma((users, ROWS))] * 2,
        compiler_params=pltpu.CompilerParams(
            collective_id=0, has_side_effects=True, vmem_limit_bytes=36 << 20
        ),
    )(
        *(
            pltpu.with_memory_space_constraint(array, pltpu.HBM)
            for array in (
                lengths,
                item_ids,
                pad_masks,
                w_dt.T,
                conv_taps,
                dt_bias.reshape(1, heads),
                decay_rates.reshape(1, heads),
                item_table,
                w_in,
                w_gate,
                w_out,
                norm_gain.reshape(1, inner),
            )
        )
    )
    return pl.pallas_call(
        final_kernel,
        name="final",
        out_shape=jax.ShapeDtypeStruct((users, 1, events, w_out.shape[1]), BF16),
        in_specs=[vmem] * 9,
        out_specs=hbm,
        scratch_shapes=[
            pltpu.VMEM((events, CHUNK), BF16),
            pltpu.VMEM((users, events, w_out.shape[1]), BF16),
            dma((users, w_out.shape[1] // CHUNK)),
        ],
        compiler_params=pltpu.CompilerParams(vmem_limit_bytes=16 << 20),
    )(carry, mix, gate, outward, columns, totals, squares, norm_gain.reshape(1, inner), w_out)


def solution(mesh):
    spans = P("batch", "col", "row")
    return jax.shard_map(
        per_device,
        mesh=mesh,
        in_specs=(spans, spans, P("batch")) + (P(),) * 9,
        out_specs=P("batch", "col", "row", None),
        check_vma=False,
    )
```

```python
import jax
import jax.numpy as jnp
from jax import lax
from jax.experimental import pallas as pl
from jax.experimental.pallas import tpu as pltpu
from jax.sharding import PartitionSpec as P

STRETCH = 128
CHUNK = 256
HALO = 16
ROWS, YS, ZS = 4, 4, 8
MESH = pl.DeviceIdType.MESH
BF16 = jnp.bfloat16
F32 = jnp.float32


def silu_of_half(v):
    return v + v * jnp.tanh(v)


def dot(a, b):
    return jnp.dot(a, b, preferred_element_type=F32)


def down_columns(row):
    return jnp.transpose(jnp.broadcast_to(row, (STRETCH, STRETCH)))


def main_kernel(
    lengths_in,
    ids_in,
    pads_in,
    w_dt_in,
    taps_in,
    bias_in,
    rates_in,
    table_in,
    w_in_in,
    w_gate_in,
    w_out_in,
    gain_in,
    carry,
    mix,
    gate,
    outward,
    columns_out,
    total_out,
    squares,
    lengths,
    ids,
    pads,
    w_dt,
    taps,
    bias,
    rates,
    table,
    w_in,
    w_gate,
    w_out,
    gain,
    half_taps,
    turned,
    gated,
    wdt_wide,
    split_steps,
    halo,
    hot,
    projected,
    joined_even,
    joined_odd,
    signal,
    in_rows,
    slopes,
    log_rows,
    step_rows,
    tails,
    running,
    states,
    logs,
    row_states,
    row_logs,
    row_before,
    z_out,
    z_states,
    z_before,
    z_log_out,
    z_logs,
    y_out,
    y_states,
    y_log_out,
    y_logs,
    c_out,
    c_states,
    back_out,
    load_sem,
    near,
    halo_send,
    halo_recv,
    x_send,
    x_recv,
    xl_send,
    xl_recv,
    z_send,
    z_recv,
    zl_send,
    zl_recv,
    y_send,
    y_recv,
    yl_send,
    yl_recv,
    c_send,
    c_recv,
    b_send,
    b_recv,
):
    users, _, events = ids.shape
    inner = w_gate.shape[1]
    heads = w_dt.shape[0]
    stretches = events // STRETCH
    shares = inner // CHUNK
    part = z_states.shape[2]
    r = lax.axis_index("row")
    col = lax.axis_index("col")
    cols_axis = lax.axis_size("col")
    y, z = col // ZS, lax.rem(col, ZS)
    first = (col * ROWS + r) * events

    def row_peer(d):
        return lax.rem(r + d, ROWS)

    def share(d, begin=0, size=CHUNK):
        return pl.ds(pl.multiple_of(row_peer(d) * CHUNK + begin, STRETCH), size)

    shares_order = (2, 1, 3, 0)
    maps = slice(inner, inner + CHUNK)
    loads = []
    pairs = [
        (ids_in, ids),
        (table_in, table),
        (w_dt_in, w_dt),
        (bias_in, bias),
        (rates_in, rates),
        (pads_in, pads),
        (lengths_in, lengths),
        (w_in_in.at[:, maps], w_in.at[:, maps]),
        (taps_in, taps),
    ]
    pairs += [(w_in_in.at[:, share(d)], w_in.at[:, share(d)]) for d in shares_order]
    pairs += [(w_gate_in, w_gate), (w_out_in.at[share(0)], w_out), (gain_in, gain)]
    for i, (source, target) in enumerate(pairs):
        loads.append(pltpu.make_async_copy(source, target, load_sem.at[i]))
        loads[-1].start()

    def z_peer(d):
        return lax.rem(z + d, ZS)

    def to_row(d):
        return {"row": row_peer(d)}

    def to_z(d):
        return {"col": y * ZS + z_peer(d)}

    def to_y(d):
        return {"col": lax.rem(y + d, YS) * ZS + z}

    next_span = {
        "row": row_peer(1),
        "col": lax.rem(col + jnp.where(r == ROWS - 1, 1, 0), cols_axis),
    }
    last_span = {
        "row": row_peer(ROWS - 1),
        "col": lax.rem(col + jnp.where(r == 0, cols_axis - 1, 0), cols_axis),
    }
    barrier = pltpu.get_barrier_semaphore()
    peers = (
        [to_row(d) for d in range(1, ROWS)]
        + [next_span, last_span]
        + [to_z(1), to_z(ZS - 1), to_y(1), to_y(YS - 1)]
    )
    for peer in peers:
        pl.semaphore_signal(barrier, inc=1, device_id=peer, device_id_type=MESH)

    def tell(index, devices):
        for device in devices:
            pl.semaphore_signal(near.at[index], inc=1, device_id=device, device_id_type=MESH)

    sides = [to_z(1), to_z(ZS - 1)]
    sent = []

    def send(src, dst, send_sem, recv_sem, device):
        copy = pltpu.make_async_remote_copy(
            src_ref=src,
            dst_ref=dst,
            send_sem=send_sem,
            recv_sem=recv_sem,
            device_id=device,
            device_id_type=MESH,
        )
        copy.start()
        sent.append(copy)
        return copy

    lanes = lax.broadcasted_iota(jnp.int32, (STRETCH, STRETCH), 1)
    lanes_f = lanes.astype(F32)
    depths = lax.broadcasted_iota(jnp.int32, (STRETCH, STRETCH), 0)
    causal = depths >= lanes

    def one_hot(row, u, begin, rows):
        column = down_columns(row)[STRETCH - rows :, :]
        for j in range(table.shape[0] // STRETCH):
            match = column == lanes_f[:rows] + float(j * STRETCH)
            hot[u, begin : begin + rows, j * STRETCH : (j + 1) * STRETCH] = jnp.where(
                match, 1.0, 0.0
            ).astype(BF16)

    wdt_wide[...] = jnp.zeros_like(wdt_wide)
    loads[0].wait()
    for u in range(users):
        for c in range(stretches):
            row = ids[u, :, c * STRETCH : (c + 1) * STRETCH].astype(F32)
            one_hot(row, u, HALO + c * STRETCH, STRETCH)

    for load in loads[1:7]:
        load.wait()
    wdt_wide[0:heads, :] = w_dt[...]
    raw = lax.dot_general(
        table[...], wdt_wide[...], (((1,), (1,)), ((), ())), preferred_element_type=F32
    )
    raw = raw + jnp.concatenate([bias[...], jnp.zeros((1, STRETCH - heads), F32)], axis=1)
    soft = jnp.maximum(raw, 0.0) + jnp.log1p(jnp.exp(-jnp.abs(raw)))
    high = soft.astype(BF16)
    split_steps[:, 0:STRETCH] = high
    split_steps[:, STRETCH:] = (soft - high.astype(F32)).astype(BF16)
    pl.semaphore_wait(barrier, len(peers))
    tail = slice(events - STRETCH, events)
    halo_copy = send(ids.at[:, :, tail], halo, halo_send, halo_recv, next_span)
    tell(0, sides)
    tell(3, [to_y(1), to_y(YS - 1)])
    for load in loads[7:10]:
        load.wait()
    half_taps[...] = 0.5 * taps[...]

    def project(slot, columns):
        projected[slot] = dot(table[...], w_in[:, columns]).astype(BF16)

    project(ROWS, maps)
    project(2, share(2))
    speed = down_columns(
        jnp.concatenate([rates[...], jnp.zeros((1, STRETCH - heads), F32)], axis=1)
    )[0:heads]
    usable = {}
    for u in range(users):
        picked = dot(hot[u, HALO:, :], split_steps[...])
        step = picked[:, 0:STRETCH] + picked[:, STRETCH:]
        for c in range(stretches):
            place = first + c * STRETCH + lax.broadcasted_iota(jnp.int32, (1, STRETCH), 1)
            rows = slice(c * STRETCH, (c + 1) * STRETCH)
            kept = jnp.logical_and(place < lengths[u], pads[u, :, rows] > 0)
            usable[u, c] = jnp.where(kept, 1.0, 0.0)
            step_t = jnp.transpose(step[rows])[0:heads] * usable[u, c]
            step_rows[u, c] = step_t
            slopes[(u * stretches + c) * heads : (u * stretches + c + 1) * heads, :] = (
                step_t * speed
            )

    gained = jnp.dot(
        slopes[...],
        jnp.where(depths <= lanes, 1.0, 0.0),
        preferred_element_type=F32,
        precision=lax.Precision.HIGHEST,
    )
    for u in range(users):
        before = [jnp.zeros((heads, 1), F32)]
        log_t = []
        for c in range(stretches):
            begin = (u * stretches + c) * heads
            log_t.append(gained[begin : begin + heads])
            before.append(before[c] + log_t[c][:, STRETCH - 1 :])
        for c in range(stretches):
            rows = slice(c * STRETCH, (c + 1) * STRETCH)
            log_rows[u, c] = log_t[c]
            so_far = before[c] + log_t[c]
            to_end = jnp.exp(so_far - before[stretches]) * step_rows[u, c]
            for h in range(heads):
                tails[u, h, :, rows] = to_end[h : h + 1, :]
            left = jnp.exp(-so_far)
            turned[u, c, 0:heads, :] = left
            turned[u, c, heads:, :] = left
            columns_out[u, rows, :] = jnp.transpose(
                jnp.concatenate(
                    [
                        log_t[c],
                        jnp.broadcast_to(usable[u, c], (heads, STRETCH)),
                        turned[u, c, pl.ds(2 * r, heads), :],
                        jnp.exp(-log_t[c]),
                        jnp.zeros((STRETCH - 4 * heads, STRETCH), F32),
                    ],
                    axis=0,
                )
            )
        for h in range(heads):
            half = h % 2
            logs[h // 2, u, :, half * STRETCH : (half + 1) * STRETCH] = jnp.broadcast_to(
                before[stretches][h : h + 1, :], (1, STRETCH)
            )
    pl.semaphore_wait(near.at[0], 2)
    tell(1, sides)
    xl_copies = [
        send(logs.at[row_peer(d)], row_logs.at[r], xl_send.at[d], xl_recv.at[d], to_row(d))
        for d in range(1, ROWS)
    ]
    row_logs[r] = logs[r]

    halo_copy.wait_recv()
    nobody = jnp.logical_and(r == 0, col == 0)
    for u in range(users):
        one_hot(jnp.where(nobody, -1.0, halo[u].astype(F32)), u, 0, HALO)

    joined = (joined_even, joined_odd)

    def gather(u, slot):
        rows = dot(hot[u], projected[slot])
        for half in range(2):
            joined[u][half] = rows[:, half * STRETCH : (half + 1) * STRETCH]

    def convolve(u, half, weights, columns):
        total = None
        for k in range(weights.shape[0]):
            begin = HALO - weights.shape[0] + 1 + k
            term = joined[u][half, begin : begin + events, :] * weights[k : k + 1, columns]
            total = term if total is None else total + term
        return total

    def make_maps(u):
        into = convolve(u, 0, taps, slice(inner, inner + STRETCH)).astype(BF16)
        outs = convolve(u, 1, taps, slice(inner + STRETCH, inner + CHUNK))
        outward[u] = outs.astype(BF16)
        for c in range(stretches):
            rows = slice(c * STRETCH, (c + 1) * STRETCH)
            in_rows[u, :, rows] = jnp.transpose(into[rows].astype(F32))

    x_copies = {}
    order = [(d, u) for d in shares_order for u in range(users)]

    def state_step(i, prefetch=True):
        d, u = order[i]
        if prefetch and i + 1 < len(order):
            gather(order[i + 1][1], order[i + 1][0])
        for half in range(2):
            columns = share(d, half * STRETCH, STRETCH)
            values = silu_of_half(convolve(u, half, half_taps, columns)).astype(BF16)
            signal[u, :, columns] = values
            scaled = (in_rows[u] * tails[u, 2 * row_peer(d) + half]).astype(BF16)
            state = dot(scaled, values).astype(BF16)
            cols = slice(half * STRETCH, (half + 1) * STRETCH)
            if d:
                states[u, d, :, cols] = state
            else:
                row_states[u, r, :, cols] = state
        if d:
            x_copies[u, d] = send(
                states.at[u, d],
                row_states.at[u, r],
                x_send.at[u, d],
                x_recv.at[u, d],
                to_row(d),
            )

    gather(0, ROWS)
    gather(1, ROWS)
    make_maps(0)
    gather(0, 2)
    make_maps(1)
    state_step(0)
    for load in loads[10:13]:
        load.wait()
    pl.semaphore_wait(near.at[1], 2)
    tell(2, sides)
    project(1, share(1))
    state_step(1)
    project(3, share(3))
    state_step(2)

    for copy in xl_copies:
        copy.wait_recv()
    block_log = row_logs[0]
    for i in range(1, ROWS):
        block_log = block_log + row_logs[i]
    z_log_out[...] = block_log
    z_logs[z] = block_log
    pl.semaphore_wait(near.at[2], 2)
    pl.semaphore_wait(near.at[3], 2)
    zl_copies = [
        send(z_log_out, z_logs.at[z], zl_send.at[d], zl_recv.at[d], to_z(d)) for d in range(1, ZS)
    ]

    project(0, share(0))
    for i in range(3, len(order)):
        state_step(i)

    for copy in zl_copies:
        copy.wait_recv()
    y_log = z_logs[0]
    for i in range(1, ZS):
        y_log = y_log + z_logs[i]
    y_log_out[...] = y_log
    y_logs[y] = y_log
    yl_copies = [
        send(y_log_out, y_logs.at[y], yl_send.at[d], yl_recv.at[d], to_y(d)) for d in range(1, YS)
    ]

    loads[13].wait()

    def gate_phase(begin, end):
        @pl.loop(begin, end)
        def _(j):
            columns = pl.ds(pl.multiple_of(j * CHUNK, CHUNK), CHUNK)
            opened = dot(table[...], w_gate[:, columns]).astype(BF16)
            opened = silu_of_half(0.5 * opened.astype(F32)).astype(BF16)
            for u in range(users):
                gate[u, :, columns] = dot(hot[u, HALO:, :], opened).astype(BF16)

    def local_phase(u, begin, end):
        @pl.loop(begin, end)
        def _(c):
            rows = pl.ds(pl.multiple_of(c * STRETCH, STRETCH), STRETCH)
            column = columns_out[u, rows, :]
            log_t = log_rows[u, c]
            step_t = step_rows[u, c]
            last = log_t[:, STRETCH - 1 :]
            tail_t = jnp.exp(log_t - last) * step_t
            stay = jnp.exp(-last)
            outs = outward[u, rows, :]
            in_t = in_rows[u, :, rows]
            scores = dot(outs, in_t.astype(BF16))
            for h in range(heads):
                cols = slice(h * STRETCH, (h + 1) * STRETCH)
                gap = jnp.where(causal, log_t[h : h + 1, :] - column[:, h : h + 1], -1e30)
                weights = (scores * jnp.exp(gap) * step_t[h : h + 1, :]).astype(BF16)
                values = signal[u, rows, cols]
                entering = jnp.where(c == 0, 0.0, running[:, cols])
                fade = column[:, 3 * heads + h : 3 * heads + h + 1]
                mix[u, rows, cols] = (
                    dot(weights, values) + dot(outs, entering.astype(BF16)) * fade
                ).astype(BF16)
                scaled = (in_t * tail_t[h : h + 1, :]).astype(BF16)
                running[:, cols] = stay[h : h + 1, :] * entering + dot(scaled, values)

    gate_phase(0, shares // 2)

    for u in range(users):
        for d in range(1, ROWS):
            x_copies[u, d].wait_recv()
        total = row_states[u, 0].astype(F32)
        for i in range(1, ROWS):
            for k in range(ZS):
                row_before[i - 1, k, u] = total[k * part : (k + 1) * part]
            total = jnp.exp(-row_logs[i, u]) * total + row_states[u, i].astype(F32)
        block = total.astype(BF16)
        for k in range(ZS):
            z_out[k, u] = block[k * part : (k + 1) * part]
    z_states[z] = z_out[z]
    z_copies = [
        send(z_out.at[z_peer(d)], z_states.at[z], z_send.at[d], z_recv.at[d], to_z(d))
        for d in (4, 3, 5, 2, 6, 1, 7)
    ]

    gate_phase(shares // 2, shares)
    local_phase(0, 0, 2)

    for copy in z_copies:
        copy.wait_recv()
    total = z_states[0].astype(F32)
    for i in range(1, ZS):
        z_before[i - 1] = total
        total = jnp.exp(-z_logs[i]) * total + z_states[i].astype(F32)
    y_out[...] = total.astype(BF16)
    y_copies = [
        send(y_out, y_states.at[y], y_send.at[d], y_recv.at[d], to_y(d)) for d in (2, 1, 3)
    ]

    local_phase(0, 2, stretches)

    for copy in yl_copies:
        copy.wait_recv()
    for copy in y_copies:
        copy.wait_recv()
    entering = jnp.zeros(y_out.shape, F32)
    for i in range(YS - 1):
        entering = jnp.where(
            i < y, jnp.exp(-y_logs[i]) * entering + y_states[i].astype(F32), entering
        )
    gone = None
    for k in range(ZS):
        value = entering
        if k:
            gone = z_logs[k - 1] if gone is None else gone + z_logs[k - 1]
            value = jnp.exp(-gone) * entering + z_before[k - 1]
        c_out[k] = value.astype(BF16)
    c_states[z] = c_out[z]
    c_copies = {
        d: send(c_out.at[z_peer(d)], c_states.at[z], c_send.at[d], c_recv.at[d], to_z(d))
        for d in (4, 3, 5, 2, 6, 1, 7)
    }

    gone = [None, row_logs[0]]
    for i in range(2, ROWS):
        gone.append(gone[-1] + row_logs[i - 1])
    kept = [None] + [jnp.exp(-gone[i]) for i in range(1, ROWS)]
    b_copies = []

    def forward(d):
        k = z_peer(ZS - d)
        value = c_states[k].astype(F32)
        back_out[0, k] = c_states[k]
        for i in range(1, ROWS):
            back_out[i, k] = (kept[i] * value + row_before[i - 1, k]).astype(BF16)
        carry[r, k] = back_out[r, k]
        for x in (2, 1, 3):
            b_copies.append(
                send(
                    back_out.at[row_peer(x), k],
                    carry.at[r, k],
                    b_send.at[x, d],
                    b_recv.at[x, d],
                    to_row(x),
                )
            )

    forward(0)
    local_phase(1, 0, 2)
    for begin, ends in ((2, (1, 7)), (3, (2, 6)), (4, (3, 5, 4))):
        for d in ends:
            c_copies[d].wait_recv()
            forward(d)
        if begin < stretches:
            local_phase(1, begin, begin + 1)

    for load in loads[14:]:
        load.wait()

    for u in range(users):
        held = carry[r, :, u].reshape(STRETCH, CHUNK)
        for c in range(stretches):
            rows = slice(c * STRETCH, (c + 1) * STRETCH)
            carried = dot(outward[u, rows, :], held)
            both = None
            for half in range(2):
                cols = share(0, half * STRETCH, STRETCH)
                place = 2 * heads + half
                value = (
                    columns_out[u, rows, place : place + 1]
                    * carried[:, half * STRETCH : (half + 1) * STRETCH]
                    + mix[u, rows, cols].astype(F32)
                ) * gate[u, rows, cols].astype(F32)
                gated[rows, half * STRETCH : (half + 1) * STRETCH] = (
                    value * gain[:, cols]
                ).astype(BF16)
                both = value * value if both is None else both + value * value
            squares[u, rows, :] = both
        for j in range(w_out.shape[1] // CHUNK):
            columns = slice(j * CHUNK, (j + 1) * CHUNK)
            total_out[u, :, columns] = dot(gated[...], w_out[:, columns])
    for copy in b_copies:
        copy.wait_recv()
    for copy in sent:
        copy.wait_send()


def final_kernel(
    carry,
    mix,
    gate,
    outward,
    columns_in,
    totals,
    partial,
    gain,
    w_out,
    result,
    gated,
    squares,
    done,
    sems,
):
    users, events, inner = mix.shape
    heads = inner // STRETCH
    width = w_out.shape[1]
    block = 2 * STRETCH
    copies = []
    scale = {}

    def owner(d, begin=0, size=CHUNK):
        place = lax.rem(lax.axis_index("row") + d, ROWS) * CHUNK + begin
        return pl.ds(pl.multiple_of(place, STRETCH), size)

    def open_gate(u, c, d):
        rows = slice(c * block, (c + 1) * block)
        held = carry[lax.rem(lax.axis_index("row") + d, ROWS), :, u].reshape(STRETCH, CHUNK)
        carried = dot(outward[u, rows, :], held)
        added = None
        for half in range(2):
            cols = owner(d, half * STRETCH, STRETCH)
            place = 2 * heads + 2 * d + half
            value = (
                columns_in[u, rows, place : place + 1]
                * carried[:, half * STRETCH : (half + 1) * STRETCH]
                + mix[u, rows, cols].astype(F32)
            ) * gate[u, rows, cols].astype(F32)
            begin = (d - 1) * CHUNK + half * STRETCH
            gated[u, rows, begin : begin + STRETCH] = (value * gain[:, cols]).astype(BF16)
            added = value * value if added is None else added + value * value
        before = partial if d == 1 else squares
        squares[u, rows, :] = before[u, rows, :] + added

    def scale_of(u):
        mean = jnp.sum(squares[u], axis=1, keepdims=True) * (1.0 / inner)
        scale[u] = lax.rsqrt(mean + 1.0) * columns_in[u, :, heads : heads + 1]

    def project(u, j):
        columns = slice(j * CHUNK, (j + 1) * CHUNK)
        values = totals[u, :, columns]
        for d in range(1, ROWS):
            values = values + dot(
                gated[u, :, (d - 1) * CHUNK : d * CHUNK], w_out[owner(d), columns]
            )
        done[u, :, columns] = (values * scale[u]).astype(BF16)

    def store(u, j):
        columns = slice(j * CHUNK, (j + 1) * CHUNK)
        copy = pltpu.make_async_copy(
            done.at[u, :, columns], result.at[u, 0, :, columns], sems.at[u, j]
        )
        copy.start()
        copies.append(copy)

    steps = [(c, d) for c in range(events // block) for d in range(1, ROWS)]
    for c, d in steps:
        open_gate(0, c, d)
    for u in range(users):
        scale_of(u)
        left = list(steps)
        for j in range(width // CHUNK):
            project(u, j)
            for _ in range(2):
                if u + 1 < users and left:
                    open_gate(u + 1, *left.pop(0))
            store(u, j)
    for copy in copies:
        copy.wait()


def per_device(
    item_ids,
    pad_masks,
    lengths,
    item_table,
    w_gate,
    w_in,
    w_dt,
    conv_taps,
    dt_bias,
    decay_rates,
    norm_gain,
    w_out,
):
    users, _, events = item_ids.shape
    items, width = item_table.shape
    inner = w_gate.shape[1]
    full = w_in.shape[1]
    heads = decay_rates.shape[0]
    stretches = events // STRETCH
    pair = 2 * STRETCH
    part = STRETCH // ZS
    vmem = pl.BlockSpec(memory_space=pltpu.VMEM)
    hbm = pl.BlockSpec(memory_space=pltpu.HBM)
    dma = pltpu.SemaphoreType.DMA
    carry, mix, gate, outward, columns, totals, squares = pl.pallas_call(
        main_kernel,
        name="main",
        out_shape=(
            jax.ShapeDtypeStruct((ROWS, ZS, users, part, pair), BF16),
            jax.ShapeDtypeStruct((users, events, inner), BF16),
            jax.ShapeDtypeStruct((users, events, inner), BF16),
            jax.ShapeDtypeStruct((users, events, STRETCH), BF16),
            jax.ShapeDtypeStruct((users, events, STRETCH), F32),
            jax.ShapeDtypeStruct((users, events, w_out.shape[1]), F32),
            jax.ShapeDtypeStruct((users, events, STRETCH), F32),
        ),
        in_specs=[hbm] * 12,
        out_specs=(vmem,) * 7,
        scratch_shapes=[
            pltpu.SMEM(lengths.shape, lengths.dtype),
            pltpu.VMEM(item_ids.shape, item_ids.dtype),
            pltpu.VMEM(pad_masks.shape, pad_masks.dtype),
            pltpu.VMEM((heads, width), BF16),
            pltpu.VMEM(conv_taps.shape, F32),
            pltpu.VMEM((1, heads), F32),
            pltpu.VMEM((1, heads), F32),
            pltpu.VMEM((items, width), BF16),
            pltpu.VMEM((width, full), BF16),
            pltpu.VMEM((width, inner), BF16),
            pltpu.VMEM((CHUNK, w_out.shape[1]), BF16),
            pltpu.VMEM((1, inner), F32),
            pltpu.VMEM(conv_taps.shape, F32),
            pltpu.VMEM((users, stretches, 2 * heads, STRETCH), F32),
            pltpu.VMEM((events, CHUNK), BF16),
            pltpu.VMEM((STRETCH, width), BF16),
            pltpu.VMEM((items, 2 * STRETCH), BF16),
            pltpu.VMEM((users, 1, STRETCH), jnp.int32),
            pltpu.VMEM((users, HALO + events, items), BF16),
            pltpu.VMEM((ROWS + 1, items, CHUNK), BF16),
            pltpu.VMEM((2, HALO + events, STRETCH), F32),
            pltpu.VMEM((2, HALO + events, STRETCH), F32),
            pltpu.VMEM((users, events, inner), BF16),
            pltpu.VMEM((users, STRETCH, events), F32),
            pltpu.VMEM((users * stretches * heads, STRETCH), F32),
            pltpu.VMEM((users, stretches, heads, STRETCH), F32),
            pltpu.VMEM((users, stretches, heads, STRETCH), F32),
            pltpu.VMEM((users, heads, 1, events), F32),
            pltpu.VMEM((STRETCH, inner), F32),
            pltpu.VMEM((users, ROWS, STRETCH, pair), BF16),
            pltpu.VMEM((ROWS, users, 1, pair), F32),
            pltpu.VMEM((users, ROWS, STRETCH, pair), BF16),
            pltpu.VMEM((ROWS, users, 1, pair), F32),
            pltpu.VMEM((ROWS - 1, ZS, users, part, pair), F32),
            pltpu.VMEM((ZS, users, part, pair), BF16),
            pltpu.VMEM((ZS, users, part, pair), BF16),
            pltpu.VMEM((ZS - 1, users, part, pair), F32),
            pltpu.VMEM((users, 1, pair), F32),
            pltpu.VMEM((ZS, users, 1, pair), F32),
            pltpu.VMEM((users, part, pair), BF16),
            pltpu.VMEM((YS, users, part, pair), BF16),
            pltpu.VMEM((users, 1, pair), F32),
            pltpu.VMEM((YS, users, 1, pair), F32),
            pltpu.VMEM((ZS, users, part, pair), BF16),
            pltpu.VMEM((ZS, users, part, pair), BF16),
            pltpu.VMEM((ROWS, ZS, users, part, pair), BF16),
            dma((16,)),
            pltpu.SemaphoreType.REGULAR((4,)),
            dma,
            dma,
        ]
        + [dma((users, ROWS))] * 2
        + [dma((ROWS,))] * 2
        + [dma((ZS,))] * 4
        + [dma((YS,))] * 4
        + [dma((ZS,))] * 2
        + [dma((ROWS, ZS))] * 2,
        compiler_params=pltpu.CompilerParams(
            collective_id=0, has_side_effects=True, vmem_limit_bytes=36 << 20
        ),
    )(
        *(
            pltpu.with_memory_space_constraint(array, pltpu.HBM)
            for array in (
                lengths,
                item_ids,
                pad_masks,
                w_dt.T,
                conv_taps,
                dt_bias.reshape(1, heads),
                decay_rates.reshape(1, heads),
                item_table,
                w_in,
                w_gate,
                w_out,
                norm_gain.reshape(1, inner),
            )
        )
    )
    return pl.pallas_call(
        final_kernel,
        name="final",
        out_shape=jax.ShapeDtypeStruct((users, 1, events, w_out.shape[1]), BF16),
        in_specs=[vmem] * 9,
        out_specs=hbm,
        scratch_shapes=[
            pltpu.VMEM((users, events, 3 * CHUNK), BF16),
            pltpu.VMEM((users, events, STRETCH), F32),
            pltpu.VMEM((users, events, w_out.shape[1]), BF16),
            dma((users, w_out.shape[1] // CHUNK)),
        ],
        compiler_params=pltpu.CompilerParams(vmem_limit_bytes=16 << 20),
    )(carry, mix, gate, outward, columns, totals, squares, norm_gain.reshape(1, inner), w_out)


def solution(mesh):
    spans = P("batch", "col", "row")
    return jax.shard_map(
        per_device,
        mesh=mesh,
        in_specs=(spans, spans, P("batch")) + (P(),) * 9,
        out_specs=P("batch", "col", "row", None),
        check_vma=False,
    )
```

```python
import jax
import jax.numpy as jnp
from jax import lax
from jax.experimental import pallas as pl
from jax.experimental.pallas import tpu as pltpu
from jax.sharding import PartitionSpec as P

STRETCH = 128
CHUNK = 256
HALO = 16
ROWS, YS, ZS = 4, 4, 8
MESH = pl.DeviceIdType.MESH
BF16 = jnp.bfloat16
F32 = jnp.float32


def silu_of_half(v):
    return v + v * jnp.tanh(v)


def dot(a, b):
    return jnp.dot(a, b, preferred_element_type=F32)


def down_columns(row):
    return jnp.transpose(jnp.broadcast_to(row, (STRETCH, STRETCH)))


def main_kernel(
    lengths_in,
    ids_in,
    pads_in,
    w_dt_in,
    taps_in,
    bias_in,
    rates_in,
    table_in,
    w_in_in,
    w_gate_in,
    w_out_in,
    gain_in,
    carry,
    mix,
    gate,
    outward,
    columns_out,
    total_out,
    squares,
    lengths,
    ids,
    pads,
    w_dt,
    taps,
    bias,
    rates,
    table,
    w_in,
    w_gate,
    w_out,
    gain,
    half_taps,
    turned,
    gated,
    wdt_wide,
    split_steps,
    halo,
    hot,
    projected,
    joined_even,
    joined_odd,
    signal,
    in_rows,
    slopes,
    log_rows,
    step_rows,
    tails,
    running,
    states,
    logs,
    row_states,
    row_logs,
    row_before,
    z_out,
    z_states,
    z_before,
    z_log_out,
    z_logs,
    y_out,
    y_states,
    y_log_out,
    y_logs,
    c_out,
    c_states,
    back_out,
    load_sem,
    near,
    halo_send,
    halo_recv,
    x_send,
    x_recv,
    xl_send,
    xl_recv,
    z_send,
    z_recv,
    zl_send,
    zl_recv,
    y_send,
    y_recv,
    yl_send,
    yl_recv,
    c_send,
    c_recv,
    b_send,
    b_recv,
):
    users, _, events = ids.shape
    inner = w_gate.shape[1]
    heads = w_dt.shape[0]
    stretches = events // STRETCH
    shares = inner // CHUNK
    part = z_states.shape[2]
    r = lax.axis_index("row")
    col = lax.axis_index("col")
    cols_axis = lax.axis_size("col")
    y, z = col // ZS, lax.rem(col, ZS)
    first = (col * ROWS + r) * events

    def row_peer(d):
        return lax.rem(r + d, ROWS)

    def share(d, begin=0, size=CHUNK):
        return pl.ds(pl.multiple_of(row_peer(d) * CHUNK + begin, STRETCH), size)

    shares_order = (2, 1, 3, 0)
    maps = slice(inner, inner + CHUNK)
    loads = []
    pairs = [
        (ids_in, ids),
        (table_in, table),
        (w_dt_in, w_dt),
        (bias_in, bias),
        (rates_in, rates),
        (pads_in, pads),
        (lengths_in, lengths),
        (w_in_in.at[:, maps], w_in.at[:, maps]),
        (taps_in, taps),
    ]
    pairs += [(w_in_in.at[:, share(d)], w_in.at[:, share(d)]) for d in shares_order]
    pairs += [(w_gate_in, w_gate), (w_out_in.at[share(0)], w_out), (gain_in, gain)]
    for i, (source, target) in enumerate(pairs):
        loads.append(pltpu.make_async_copy(source, target, load_sem.at[i]))
        loads[-1].start()

    def z_peer(d):
        return lax.rem(z + d, ZS)

    def to_row(d):
        return {"row": row_peer(d)}

    def to_z(d):
        return {"col": y * ZS + z_peer(d)}

    def to_y(d):
        return {"col": lax.rem(y + d, YS) * ZS + z}

    next_span = {
        "row": row_peer(1),
        "col": lax.rem(col + jnp.where(r == ROWS - 1, 1, 0), cols_axis),
    }
    last_span = {
        "row": row_peer(ROWS - 1),
        "col": lax.rem(col + jnp.where(r == 0, cols_axis - 1, 0), cols_axis),
    }
    barrier = pltpu.get_barrier_semaphore()
    peers = (
        [to_row(d) for d in range(1, ROWS)]
        + [next_span, last_span]
        + [to_z(1), to_z(ZS - 1), to_y(1), to_y(YS - 1)]
    )
    for peer in peers:
        pl.semaphore_signal(barrier, inc=1, device_id=peer, device_id_type=MESH)

    def tell(index, devices):
        for device in devices:
            pl.semaphore_signal(near.at[index], inc=1, device_id=device, device_id_type=MESH)

    sides = [to_z(1), to_z(ZS - 1)]
    sent = []

    def send(src, dst, send_sem, recv_sem, device):
        copy = pltpu.make_async_remote_copy(
            src_ref=src,
            dst_ref=dst,
            send_sem=send_sem,
            recv_sem=recv_sem,
            device_id=device,
            device_id_type=MESH,
        )
        copy.start()
        sent.append(copy)
        return copy

    lanes = lax.broadcasted_iota(jnp.int32, (STRETCH, STRETCH), 1)
    lanes_f = lanes.astype(F32)
    depths = lax.broadcasted_iota(jnp.int32, (STRETCH, STRETCH), 0)
    causal = depths >= lanes

    def one_hot(row, u, begin, rows):
        column = down_columns(row)[STRETCH - rows :, :]
        for j in range(table.shape[0] // STRETCH):
            match = column == lanes_f[:rows] + float(j * STRETCH)
            hot[u, begin : begin + rows, j * STRETCH : (j + 1) * STRETCH] = jnp.where(
                match, 1.0, 0.0
            ).astype(BF16)

    wdt_wide[...] = jnp.zeros_like(wdt_wide)
    loads[0].wait()
    for u in range(users):
        for c in range(stretches):
            row = ids[u, :, c * STRETCH : (c + 1) * STRETCH].astype(F32)
            one_hot(row, u, HALO + c * STRETCH, STRETCH)

    for load in loads[1:7]:
        load.wait()
    wdt_wide[0:heads, :] = w_dt[...]
    raw = lax.dot_general(
        table[...], wdt_wide[...], (((1,), (1,)), ((), ())), preferred_element_type=F32
    )
    raw = raw + jnp.concatenate([bias[...], jnp.zeros((1, STRETCH - heads), F32)], axis=1)
    soft = jnp.maximum(raw, 0.0) + jnp.log1p(jnp.exp(-jnp.abs(raw)))
    high = soft.astype(BF16)
    split_steps[:, 0:STRETCH] = high
    split_steps[:, STRETCH:] = (soft - high.astype(F32)).astype(BF16)
    pl.semaphore_wait(barrier, len(peers))
    tail = slice(events - STRETCH, events)
    halo_copy = send(ids.at[:, :, tail], halo, halo_send, halo_recv, next_span)
    tell(0, sides)
    tell(3, [to_y(1), to_y(YS - 1)])
    for load in loads[7:10]:
        load.wait()
    half_taps[...] = 0.5 * taps[...]

    def project(slot, columns):
        projected[slot] = dot(table[...], w_in[:, columns]).astype(BF16)

    project(ROWS, maps)
    project(2, share(2))
    speed = down_columns(
        jnp.concatenate([rates[...], jnp.zeros((1, STRETCH - heads), F32)], axis=1)
    )[0:heads]
    usable = {}
    for u in range(users):
        picked = dot(hot[u, HALO:, :], split_steps[...])
        step = picked[:, 0:STRETCH] + picked[:, STRETCH:]
        for c in range(stretches):
            place = first + c * STRETCH + lax.broadcasted_iota(jnp.int32, (1, STRETCH), 1)
            rows = slice(c * STRETCH, (c + 1) * STRETCH)
            kept = jnp.logical_and(place < lengths[u], pads[u, :, rows] > 0)
            usable[u, c] = jnp.where(kept, 1.0, 0.0)
            step_t = jnp.transpose(step[rows])[0:heads] * usable[u, c]
            step_rows[u, c] = step_t
            slopes[(u * stretches + c) * heads : (u * stretches + c + 1) * heads, :] = (
                step_t * speed
            )

    gained = jnp.dot(
        slopes[...],
        jnp.where(depths <= lanes, 1.0, 0.0),
        preferred_element_type=F32,
        precision=lax.Precision.HIGHEST,
    )
    for u in range(users):
        before = [jnp.zeros((heads, 1), F32)]
        log_t = []
        for c in range(stretches):
            begin = (u * stretches + c) * heads
            log_t.append(gained[begin : begin + heads])
            before.append(before[c] + log_t[c][:, STRETCH - 1 :])
        for c in range(stretches):
            rows = slice(c * STRETCH, (c + 1) * STRETCH)
            log_rows[u, c] = log_t[c]
            so_far = before[c] + log_t[c]
            to_end = jnp.exp(so_far - before[stretches]) * step_rows[u, c]
            for h in range(heads):
                tails[u, h, :, rows] = to_end[h : h + 1, :]
            left = jnp.exp(-so_far)
            turned[u, c, 0:heads, :] = left
            turned[u, c, heads:, :] = left
            columns_out[u, rows, :] = jnp.transpose(
                jnp.concatenate(
                    [
                        log_t[c],
                        jnp.broadcast_to(usable[u, c], (heads, STRETCH)),
                        turned[u, c, pl.ds(2 * r, heads), :],
                        jnp.exp(-log_t[c]),
                        jnp.zeros((STRETCH - 4 * heads, STRETCH), F32),
                    ],
                    axis=0,
                )
            )
        for h in range(heads):
            half = h % 2
            logs[h // 2, u, :, half * STRETCH : (half + 1) * STRETCH] = jnp.broadcast_to(
                before[stretches][h : h + 1, :], (1, STRETCH)
            )
    pl.semaphore_wait(near.at[0], 2)
    tell(1, sides)
    xl_copies = [
        send(logs.at[row_peer(d)], row_logs.at[r], xl_send.at[d], xl_recv.at[d], to_row(d))
        for d in range(1, ROWS)
    ]
    row_logs[r] = logs[r]

    for load in loads[10:13]:
        load.wait()
    for d in (1, 3, 0):
        project(d, share(d))
    pl.semaphore_wait(near.at[1], 2)
    tell(2, sides)

    halo_copy.wait_recv()
    nobody = jnp.logical_and(r == 0, col == 0)
    for u in range(users):
        one_hot(jnp.where(nobody, -1.0, halo[u].astype(F32)), u, 0, HALO)

    joined = (joined_even, joined_odd)

    def gather(u, slot):
        rows = dot(hot[u], projected[slot])
        for half in range(2):
            joined[u][half] = rows[:, half * STRETCH : (half + 1) * STRETCH]

    def convolve(u, half, weights, columns):
        total = None
        for k in range(weights.shape[0]):
            begin = HALO - weights.shape[0] + 1 + k
            term = joined[u][half, begin : begin + events, :] * weights[k : k + 1, columns]
            total = term if total is None else total + term
        return total

    def make_maps(u):
        into = convolve(u, 0, taps, slice(inner, inner + STRETCH)).astype(BF16)
        outs = convolve(u, 1, taps, slice(inner + STRETCH, inner + CHUNK))
        outward[u] = outs.astype(BF16)
        for c in range(stretches):
            rows = slice(c * STRETCH, (c + 1) * STRETCH)
            in_rows[u, :, rows] = jnp.transpose(into[rows].astype(F32))

    x_copies = {}
    order = [(d, u) for d in shares_order for u in range(users)]

    def state_step(i, prefetch=True):
        d, u = order[i]
        if prefetch and i + 1 < len(order):
            gather(order[i + 1][1], order[i + 1][0])
        for half in range(2):
            columns = share(d, half * STRETCH, STRETCH)
            values = silu_of_half(convolve(u, half, half_taps, columns)).astype(BF16)
            signal[u, :, columns] = values
            scaled = (in_rows[u] * tails[u, 2 * row_peer(d) + half]).astype(BF16)
            state = dot(scaled, values).astype(BF16)
            cols = slice(half * STRETCH, (half + 1) * STRETCH)
            if d:
                states[u, d, :, cols] = state
            else:
                row_states[u, r, :, cols] = state
        if d:
            x_copies[u, d] = send(
                states.at[u, d],
                row_states.at[u, r],
                x_send.at[u, d],
                x_recv.at[u, d],
                to_row(d),
            )

    gather(0, ROWS)
    gather(1, ROWS)
    make_maps(0)
    gather(0, 2)
    make_maps(1)
    for i in range(3):
        state_step(i)

    for copy in xl_copies:
        copy.wait_recv()
    block_log = row_logs[0]
    for i in range(1, ROWS):
        block_log = block_log + row_logs[i]
    z_log_out[...] = block_log
    z_logs[z] = block_log
    pl.semaphore_wait(near.at[2], 2)
    pl.semaphore_wait(near.at[3], 2)
    zl_copies = [
        send(z_log_out, z_logs.at[z], zl_send.at[d], zl_recv.at[d], to_z(d)) for d in range(1, ZS)
    ]

    for i in range(3, len(order)):
        state_step(i)

    loads[13].wait()

    def gate_phase(begin, end):
        @pl.loop(begin, end)
        def _(j):
            columns = pl.ds(pl.multiple_of(j * CHUNK, CHUNK), CHUNK)
            opened = dot(table[...], w_gate[:, columns]).astype(BF16)
            opened = silu_of_half(0.5 * opened.astype(F32)).astype(BF16)
            for u in range(users):
                gate[u, :, columns] = dot(hot[u, HALO:, :], opened).astype(BF16)

    def local_phase(u, begin, end):
        @pl.loop(begin, end)
        def _(c):
            rows = pl.ds(pl.multiple_of(c * STRETCH, STRETCH), STRETCH)
            column = columns_out[u, rows, :]
            log_t = log_rows[u, c]
            step_t = step_rows[u, c]
            last = log_t[:, STRETCH - 1 :]
            tail_t = jnp.exp(log_t - last) * step_t
            stay = jnp.exp(-last)
            outs = outward[u, rows, :]
            in_t = in_rows[u, :, rows]
            scores = dot(outs, in_t.astype(BF16))
            for h in range(heads):
                cols = slice(h * STRETCH, (h + 1) * STRETCH)
                gap = jnp.where(causal, log_t[h : h + 1, :] - column[:, h : h + 1], -1e30)
                weights = (scores * jnp.exp(gap) * step_t[h : h + 1, :]).astype(BF16)
                values = signal[u, rows, cols]
                entering = jnp.where(c == 0, 0.0, running[:, cols])
                fade = column[:, 3 * heads + h : 3 * heads + h + 1]
                mix[u, rows, cols] = (
                    dot(weights, values) + dot(outs, entering.astype(BF16)) * fade
                ).astype(BF16)
                scaled = (in_t * tail_t[h : h + 1, :]).astype(BF16)
                running[:, cols] = stay[h : h + 1, :] * entering + dot(scaled, values)

    gate_phase(0, shares // 2)

    for u in range(users):
        for d in range(1, ROWS):
            x_copies[u, d].wait_recv()
        total = row_states[u, 0].astype(F32)
        for i in range(1, ROWS):
            for k in range(ZS):
                row_before[i - 1, k, u] = total[k * part : (k + 1) * part]
            total = jnp.exp(-row_logs[i, u]) * total + row_states[u, i].astype(F32)
        block = total.astype(BF16)
        for k in range(ZS):
            z_out[k, u] = block[k * part : (k + 1) * part]
    z_states[z] = z_out[z]
    z_copies = [
        send(z_out.at[z_peer(d)], z_states.at[z], z_send.at[d], z_recv.at[d], to_z(d))
        for d in (4, 3, 5, 2, 6, 1, 7)
    ]

    gate_phase(shares // 2, shares)
    local_phase(0, 0, 3)

    for copy in zl_copies:
        copy.wait_recv()
    y_log = z_logs[0]
    for i in range(1, ZS):
        y_log = y_log + z_logs[i]
    y_log_out[...] = y_log
    y_logs[y] = y_log
    yl_copies = [
        send(y_log_out, y_logs.at[y], yl_send.at[d], yl_recv.at[d], to_y(d)) for d in range(1, YS)
    ]

    for copy in z_copies:
        copy.wait_recv()
    total = z_states[0].astype(F32)
    for i in range(1, ZS):
        z_before[i - 1] = total
        total = jnp.exp(-z_logs[i]) * total + z_states[i].astype(F32)
    y_out[...] = total.astype(BF16)
    y_copies = [
        send(y_out, y_states.at[y], y_send.at[d], y_recv.at[d], to_y(d)) for d in (2, 1, 3)
    ]

    local_phase(0, 3, stretches)
    local_phase(1, 0, 2)

    for copy in yl_copies:
        copy.wait_recv()
    for copy in y_copies:
        copy.wait_recv()
    entering = jnp.zeros(y_out.shape, F32)
    for i in range(YS - 1):
        entering = jnp.where(
            i < y, jnp.exp(-y_logs[i]) * entering + y_states[i].astype(F32), entering
        )
    gone = None
    for k in range(ZS):
        value = entering
        if k:
            gone = z_logs[k - 1] if gone is None else gone + z_logs[k - 1]
            value = jnp.exp(-gone) * entering + z_before[k - 1]
        c_out[k] = value.astype(BF16)
    c_states[z] = c_out[z]
    c_copies = {
        d: send(c_out.at[z_peer(d)], c_states.at[z], c_send.at[d], c_recv.at[d], to_z(d))
        for d in (4, 3, 5, 2, 6, 1, 7)
    }

    gone = [None, row_logs[0]]
    for i in range(2, ROWS):
        gone.append(gone[-1] + row_logs[i - 1])
    kept = [None] + [jnp.exp(-gone[i]) for i in range(1, ROWS)]
    b_copies = []

    def forward(d):
        k = z_peer(ZS - d)
        value = c_states[k].astype(F32)
        back_out[0, k] = c_states[k]
        for i in range(1, ROWS):
            back_out[i, k] = (kept[i] * value + row_before[i - 1, k]).astype(BF16)
        carry[r, k] = back_out[r, k]
        for x in (2, 1, 3):
            b_copies.append(
                send(
                    back_out.at[row_peer(x), k],
                    carry.at[r, k],
                    b_send.at[x, d],
                    b_recv.at[x, d],
                    to_row(x),
                )
            )

    forward(0)
    local_phase(1, 2, 3)
    for begin, ends in ((3, (1, 7)), (4, (2, 6)), (4, (3, 5, 4))):
        for d in ends:
            c_copies[d].wait_recv()
            forward(d)
        if begin < stretches:
            local_phase(1, begin, begin + 1)

    for load in loads[14:]:
        load.wait()

    for u in range(users):
        held = carry[r, :, u].reshape(STRETCH, CHUNK)
        for c in range(stretches):
            rows = slice(c * STRETCH, (c + 1) * STRETCH)
            carried = dot(outward[u, rows, :], held)
            both = None
            for half in range(2):
                cols = share(0, half * STRETCH, STRETCH)
                place = 2 * heads + half
                value = (
                    columns_out[u, rows, place : place + 1]
                    * carried[:, half * STRETCH : (half + 1) * STRETCH]
                    + mix[u, rows, cols].astype(F32)
                ) * gate[u, rows, cols].astype(F32)
                gated[rows, half * STRETCH : (half + 1) * STRETCH] = (
                    value * gain[:, cols]
                ).astype(BF16)
                both = value * value if both is None else both + value * value
            squares[u, rows, :] = both
        for j in range(w_out.shape[1] // CHUNK):
            columns = slice(j * CHUNK, (j + 1) * CHUNK)
            total_out[u, :, columns] = dot(gated[...], w_out[:, columns])
    for copy in b_copies:
        copy.wait_recv()
    for copy in sent:
        copy.wait_send()


def final_kernel(
    carry,
    mix,
    gate,
    outward,
    columns_in,
    totals,
    partial,
    gain,
    w_out,
    result,
    gated,
    squares,
    done,
    sems,
):
    users, events, inner = mix.shape
    heads = inner // STRETCH
    width = w_out.shape[1]
    block = 2 * STRETCH
    copies = []
    scale = {}

    def owner(d, begin=0, size=CHUNK):
        place = lax.rem(lax.axis_index("row") + d, ROWS) * CHUNK + begin
        return pl.ds(pl.multiple_of(place, STRETCH), size)

    def open_gate(u, c, d):
        rows = slice(c * block, (c + 1) * block)
        held = carry[lax.rem(lax.axis_index("row") + d, ROWS), :, u].reshape(STRETCH, CHUNK)
        carried = dot(outward[u, rows, :], held)
        added = None
        for half in range(2):
            cols = owner(d, half * STRETCH, STRETCH)
            place = 2 * heads + 2 * d + half
            value = (
                columns_in[u, rows, place : place + 1]
                * carried[:, half * STRETCH : (half + 1) * STRETCH]
                + mix[u, rows, cols].astype(F32)
            ) * gate[u, rows, cols].astype(F32)
            begin = (d - 1) * CHUNK + half * STRETCH
            gated[u, rows, begin : begin + STRETCH] = (value * gain[:, cols]).astype(BF16)
            added = value * value if added is None else added + value * value
        before = partial if d == 1 else squares
        squares[u, rows, :] = before[u, rows, :] + added

    def scale_of(u):
        mean = jnp.sum(squares[u], axis=1, keepdims=True) * (1.0 / inner)
        scale[u] = lax.rsqrt(mean + 1.0) * columns_in[u, :, heads : heads + 1]

    def project(u, j):
        columns = slice(j * CHUNK, (j + 1) * CHUNK)
        values = totals[u, :, columns]
        for d in range(1, ROWS):
            values = values + dot(
                gated[u, :, (d - 1) * CHUNK : d * CHUNK], w_out[owner(d), columns]
            )
        done[u, :, columns] = (values * scale[u]).astype(BF16)

    def store(u, j):
        columns = slice(j * CHUNK, (j + 1) * CHUNK)
        copy = pltpu.make_async_copy(
            done.at[u, :, columns], result.at[u, 0, :, columns], sems.at[u, j]
        )
        copy.start()
        copies.append(copy)

    steps = [(c, d) for c in range(events // block) for d in range(1, ROWS)]
    for c, d in steps:
        open_gate(0, c, d)
    for u in range(users):
        scale_of(u)
        left = list(steps)
        for j in range(width // CHUNK):
            project(u, j)
            for _ in range(2):
                if u + 1 < users and left:
                    open_gate(u + 1, *left.pop(0))
            store(u, j)
    for copy in copies:
        copy.wait()


def per_device(
    item_ids,
    pad_masks,
    lengths,
    item_table,
    w_gate,
    w_in,
    w_dt,
    conv_taps,
    dt_bias,
    decay_rates,
    norm_gain,
    w_out,
):
    users, _, events = item_ids.shape
    items, width = item_table.shape
    inner = w_gate.shape[1]
    full = w_in.shape[1]
    heads = decay_rates.shape[0]
    stretches = events // STRETCH
    pair = 2 * STRETCH
    part = STRETCH // ZS
    vmem = pl.BlockSpec(memory_space=pltpu.VMEM)
    hbm = pl.BlockSpec(memory_space=pltpu.HBM)
    dma = pltpu.SemaphoreType.DMA
    carry, mix, gate, outward, columns, totals, squares = pl.pallas_call(
        main_kernel,
        name="main",
        out_shape=(
            jax.ShapeDtypeStruct((ROWS, ZS, users, part, pair), BF16),
            jax.ShapeDtypeStruct((users, events, inner), BF16),
            jax.ShapeDtypeStruct((users, events, inner), BF16),
            jax.ShapeDtypeStruct((users, events, STRETCH), BF16),
            jax.ShapeDtypeStruct((users, events, STRETCH), F32),
            jax.ShapeDtypeStruct((users, events, w_out.shape[1]), F32),
            jax.ShapeDtypeStruct((users, events, STRETCH), F32),
        ),
        in_specs=[hbm] * 12,
        out_specs=(vmem,) * 7,
        scratch_shapes=[
            pltpu.SMEM(lengths.shape, lengths.dtype),
            pltpu.VMEM(item_ids.shape, item_ids.dtype),
            pltpu.VMEM(pad_masks.shape, pad_masks.dtype),
            pltpu.VMEM((heads, width), BF16),
            pltpu.VMEM(conv_taps.shape, F32),
            pltpu.VMEM((1, heads), F32),
            pltpu.VMEM((1, heads), F32),
            pltpu.VMEM((items, width), BF16),
            pltpu.VMEM((width, full), BF16),
            pltpu.VMEM((width, inner), BF16),
            pltpu.VMEM((CHUNK, w_out.shape[1]), BF16),
            pltpu.VMEM((1, inner), F32),
            pltpu.VMEM(conv_taps.shape, F32),
            pltpu.VMEM((users, stretches, 2 * heads, STRETCH), F32),
            pltpu.VMEM((events, CHUNK), BF16),
            pltpu.VMEM((STRETCH, width), BF16),
            pltpu.VMEM((items, 2 * STRETCH), BF16),
            pltpu.VMEM((users, 1, STRETCH), jnp.int32),
            pltpu.VMEM((users, HALO + events, items), BF16),
            pltpu.VMEM((ROWS + 1, items, CHUNK), BF16),
            pltpu.VMEM((2, HALO + events, STRETCH), F32),
            pltpu.VMEM((2, HALO + events, STRETCH), F32),
            pltpu.VMEM((users, events, inner), BF16),
            pltpu.VMEM((users, STRETCH, events), F32),
            pltpu.VMEM((users * stretches * heads, STRETCH), F32),
            pltpu.VMEM((users, stretches, heads, STRETCH), F32),
            pltpu.VMEM((users, stretches, heads, STRETCH), F32),
            pltpu.VMEM((users, heads, 1, events), F32),
            pltpu.VMEM((STRETCH, inner), F32),
            pltpu.VMEM((users, ROWS, STRETCH, pair), BF16),
            pltpu.VMEM((ROWS, users, 1, pair), F32),
            pltpu.VMEM((users, ROWS, STRETCH, pair), BF16),
            pltpu.VMEM((ROWS, users, 1, pair), F32),
            pltpu.VMEM((ROWS - 1, ZS, users, part, pair), F32),
            pltpu.VMEM((ZS, users, part, pair), BF16),
            pltpu.VMEM((ZS, users, part, pair), BF16),
            pltpu.VMEM((ZS - 1, users, part, pair), F32),
            pltpu.VMEM((users, 1, pair), F32),
            pltpu.VMEM((ZS, users, 1, pair), F32),
            pltpu.VMEM((users, part, pair), BF16),
            pltpu.VMEM((YS, users, part, pair), BF16),
            pltpu.VMEM((users, 1, pair), F32),
            pltpu.VMEM((YS, users, 1, pair), F32),
            pltpu.VMEM((ZS, users, part, pair), BF16),
            pltpu.VMEM((ZS, users, part, pair), BF16),
            pltpu.VMEM((ROWS, ZS, users, part, pair), BF16),
            dma((16,)),
            pltpu.SemaphoreType.REGULAR((4,)),
            dma,
            dma,
        ]
        + [dma((users, ROWS))] * 2
        + [dma((ROWS,))] * 2
        + [dma((ZS,))] * 4
        + [dma((YS,))] * 4
        + [dma((ZS,))] * 2
        + [dma((ROWS, ZS))] * 2,
        compiler_params=pltpu.CompilerParams(
            collective_id=0, has_side_effects=True, vmem_limit_bytes=36 << 20
        ),
    )(
        *(
            pltpu.with_memory_space_constraint(array, pltpu.HBM)
            for array in (
                lengths,
                item_ids,
                pad_masks,
                w_dt.T,
                conv_taps,
                dt_bias.reshape(1, heads),
                decay_rates.reshape(1, heads),
                item_table,
                w_in,
                w_gate,
                w_out,
                norm_gain.reshape(1, inner),
            )
        )
    )
    return pl.pallas_call(
        final_kernel,
        name="final",
        out_shape=jax.ShapeDtypeStruct((users, 1, events, w_out.shape[1]), BF16),
        in_specs=[vmem] * 9,
        out_specs=hbm,
        scratch_shapes=[
            pltpu.VMEM((users, events, 3 * CHUNK), BF16),
            pltpu.VMEM((users, events, STRETCH), F32),
            pltpu.VMEM((users, events, w_out.shape[1]), BF16),
            dma((users, w_out.shape[1] // CHUNK)),
        ],
        compiler_params=pltpu.CompilerParams(vmem_limit_bytes=16 << 20),
    )(carry, mix, gate, outward, columns, totals, squares, norm_gain.reshape(1, inner), w_out)


def solution(mesh):
    spans = P("batch", "col", "row")
    return jax.shard_map(
        per_device,
        mesh=mesh,
        in_specs=(spans, spans, P("batch")) + (P(),) * 9,
        out_specs=P("batch", "col", "row", None),
        check_vma=False,
    )
```

```python
import jax
import jax.numpy as jnp
from jax import lax
from jax.experimental import pallas as pl
from jax.experimental.pallas import tpu as pltpu
from jax.sharding import PartitionSpec as P

STRETCH = 128
CHUNK = 256
WIDE = 512
HALO = 16
ROWS, YS, ZS = 4, 4, 8
MESH = pl.DeviceIdType.MESH
BF16 = jnp.bfloat16
F32 = jnp.float32


def silu_of_half(v):
    return v + v * jnp.tanh(v)


def dot(a, b):
    return jnp.dot(a, b, preferred_element_type=F32)


def down_columns(row):
    return jnp.transpose(jnp.broadcast_to(row, (STRETCH, STRETCH)))


def main_kernel(
    lengths_in,
    ids_in,
    pads_in,
    w_dt_in,
    taps_in,
    bias_in,
    rates_in,
    table_in,
    w_in_in,
    w_gate_in,
    w_out_in,
    gain_in,
    carry,
    mix,
    gate,
    outward,
    columns_out,
    total_out,
    squares,
    lengths,
    ids,
    pads,
    w_dt,
    taps,
    bias,
    rates,
    table,
    w_in,
    w_gate,
    w_out,
    gain,
    half_taps,
    turned,
    gated,
    wdt_wide,
    split_steps,
    halo,
    hot,
    projected,
    joined_even,
    joined_odd,
    signal,
    in_rows,
    slopes,
    log_rows,
    step_rows,
    tails,
    running,
    states,
    logs,
    row_states,
    row_logs,
    row_before,
    z_out,
    z_states,
    z_before,
    z_log_out,
    z_logs,
    y_out,
    y_states,
    y_log_out,
    y_logs,
    c_out,
    c_states,
    back_out,
    load_sem,
    near,
    halo_send,
    halo_recv,
    x_send,
    x_recv,
    xl_send,
    xl_recv,
    z_send,
    z_recv,
    zl_send,
    zl_recv,
    y_send,
    y_recv,
    yl_send,
    yl_recv,
    c_send,
    c_recv,
    b_send,
    b_recv,
):
    users, _, events = ids.shape
    inner = w_gate.shape[1]
    heads = w_dt.shape[0]
    stretches = events // STRETCH
    part = z_states.shape[2]
    r = lax.axis_index("row")
    col = lax.axis_index("col")
    cols_axis = lax.axis_size("col")
    y, z = col // ZS, lax.rem(col, ZS)
    first = (col * ROWS + r) * events

    def row_peer(d):
        return lax.rem(r + d, ROWS)

    def share(d, begin=0, size=CHUNK):
        return pl.ds(pl.multiple_of(row_peer(d) * CHUNK + begin, STRETCH), size)

    shares_order = (2, 1, 3, 0)
    maps = slice(inner, inner + CHUNK)
    loads = []
    pairs = [
        (ids_in, ids),
        (table_in, table),
        (w_dt_in, w_dt),
        (bias_in, bias),
        (rates_in, rates),
        (pads_in, pads),
        (lengths_in, lengths),
        (w_in_in.at[:, maps], w_in.at[:, maps]),
        (taps_in, taps),
    ]
    pairs += [(w_in_in.at[:, share(d)], w_in.at[:, share(d)]) for d in shares_order]
    pairs += [(w_gate_in, w_gate), (w_out_in.at[share(0)], w_out), (gain_in, gain)]
    for i, (source, target) in enumerate(pairs):
        loads.append(pltpu.make_async_copy(source, target, load_sem.at[i]))
        loads[-1].start()

    def z_peer(d):
        return lax.rem(z + d, ZS)

    def to_row(d):
        return {"row": row_peer(d)}

    def to_z(d):
        return {"col": y * ZS + z_peer(d)}

    def to_y(d):
        return {"col": lax.rem(y + d, YS) * ZS + z}

    next_span = {
        "row": row_peer(1),
        "col": lax.rem(col + jnp.where(r == ROWS - 1, 1, 0), cols_axis),
    }
    last_span = {
        "row": row_peer(ROWS - 1),
        "col": lax.rem(col + jnp.where(r == 0, cols_axis - 1, 0), cols_axis),
    }
    barrier = pltpu.get_barrier_semaphore()
    peers = (
        [to_row(d) for d in range(1, ROWS)]
        + [next_span, last_span]
        + [to_z(1), to_z(ZS - 1), to_y(1), to_y(YS - 1)]
    )
    for peer in peers:
        pl.semaphore_signal(barrier, inc=1, device_id=peer, device_id_type=MESH)

    def tell(index, devices):
        for device in devices:
            pl.semaphore_signal(near.at[index], inc=1, device_id=device, device_id_type=MESH)

    sides = [to_z(1), to_z(ZS - 1)]
    sent = []

    def send(src, dst, send_sem, recv_sem, device):
        copy = pltpu.make_async_remote_copy(
            src_ref=src,
            dst_ref=dst,
            send_sem=send_sem,
            recv_sem=recv_sem,
            device_id=device,
            device_id_type=MESH,
        )
        copy.start()
        sent.append(copy)
        return copy

    lanes = lax.broadcasted_iota(jnp.int32, (STRETCH, STRETCH), 1)
    lanes_f = lanes.astype(F32)
    depths = lax.broadcasted_iota(jnp.int32, (STRETCH, STRETCH), 0)
    causal = depths >= lanes

    def one_hot(row, u, begin, rows):
        column = down_columns(row)[STRETCH - rows :, :]
        for j in range(table.shape[0] // STRETCH):
            match = column == lanes_f[:rows] + float(j * STRETCH)
            hot[u, begin : begin + rows, j * STRETCH : (j + 1) * STRETCH] = jnp.where(
                match, 1.0, 0.0
            ).astype(BF16)

    wdt_wide[...] = jnp.zeros_like(wdt_wide)
    loads[0].wait()
    for u in range(users):
        for c in range(stretches):
            row = ids[u, :, c * STRETCH : (c + 1) * STRETCH].astype(F32)
            one_hot(row, u, HALO + c * STRETCH, STRETCH)

    for load in loads[1:7]:
        load.wait()
    wdt_wide[0:heads, :] = w_dt[...]
    raw = lax.dot_general(
        table[...], wdt_wide[...], (((1,), (1,)), ((), ())), preferred_element_type=F32
    )
    raw = raw + jnp.concatenate([bias[...], jnp.zeros((1, STRETCH - heads), F32)], axis=1)
    soft = jnp.maximum(raw, 0.0) + jnp.log1p(jnp.exp(-jnp.abs(raw)))
    high = soft.astype(BF16)
    split_steps[:, 0:STRETCH] = high
    split_steps[:, STRETCH:] = (soft - high.astype(F32)).astype(BF16)
    pl.semaphore_wait(barrier, len(peers))
    tail = slice(events - STRETCH, events)
    halo_copy = send(ids.at[:, :, tail], halo, halo_send, halo_recv, next_span)
    tell(0, sides)
    tell(3, [to_y(1), to_y(YS - 1)])
    for load in loads[7:10]:
        load.wait()
    half_taps[...] = 0.5 * taps[...]

    def project(slot, columns):
        projected[slot] = dot(table[...], w_in[:, columns]).astype(BF16)

    project(ROWS, maps)
    project(2, share(2))
    speed = down_columns(
        jnp.concatenate([rates[...], jnp.zeros((1, STRETCH - heads), F32)], axis=1)
    )[0:heads]
    usable = {}
    for u in range(users):
        picked = dot(hot[u, HALO:, :], split_steps[...])
        step = picked[:, 0:STRETCH] + picked[:, STRETCH:]
        for c in range(stretches):
            place = first + c * STRETCH + lax.broadcasted_iota(jnp.int32, (1, STRETCH), 1)
            rows = slice(c * STRETCH, (c + 1) * STRETCH)
            kept = jnp.logical_and(place < lengths[u], pads[u, :, rows] > 0)
            usable[u, c] = jnp.where(kept, 1.0, 0.0)
            step_t = jnp.transpose(step[rows])[0:heads] * usable[u, c]
            step_rows[u, c] = step_t
            slopes[(u * stretches + c) * heads : (u * stretches + c + 1) * heads, :] = (
                step_t * speed
            )

    gained = jnp.dot(
        slopes[...],
        jnp.where(depths <= lanes, 1.0, 0.0),
        preferred_element_type=F32,
        precision=lax.Precision.HIGHEST,
    )
    for u in range(users):
        before = [jnp.zeros((heads, 1), F32)]
        log_t = []
        for c in range(stretches):
            begin = (u * stretches + c) * heads
            log_t.append(gained[begin : begin + heads])
            before.append(before[c] + log_t[c][:, STRETCH - 1 :])
        for c in range(stretches):
            rows = slice(c * STRETCH, (c + 1) * STRETCH)
            log_rows[u, c] = log_t[c]
            so_far = before[c] + log_t[c]
            to_end = jnp.exp(so_far - before[stretches]) * step_rows[u, c]
            for h in range(heads):
                tails[u, h, :, rows] = to_end[h : h + 1, :]
            left = jnp.exp(-so_far)
            turned[u, c, 0:heads, :] = left
            turned[u, c, heads:, :] = left
            columns_out[u, rows, :] = jnp.transpose(
                jnp.concatenate(
                    [
                        log_t[c],
                        jnp.broadcast_to(usable[u, c], (heads, STRETCH)),
                        turned[u, c, pl.ds(2 * r, heads), :],
                        jnp.exp(-log_t[c]),
                        jnp.zeros((STRETCH - 4 * heads, STRETCH), F32),
                    ],
                    axis=0,
                )
            )
        for h in range(heads):
            half = h % 2
            logs[h // 2, u, :, half * STRETCH : (half + 1) * STRETCH] = jnp.broadcast_to(
                before[stretches][h : h + 1, :], (1, STRETCH)
            )
    pl.semaphore_wait(near.at[0], 2)
    tell(1, sides)
    xl_copies = [
        send(logs.at[row_peer(d)], row_logs.at[r], xl_send.at[d], xl_recv.at[d], to_row(d))
        for d in range(1, ROWS)
    ]
    row_logs[r] = logs[r]

    for load in loads[10:13]:
        load.wait()
    for d in (1, 3, 0):
        project(d, share(d))
    pl.semaphore_wait(near.at[1], 2)
    tell(2, sides)

    halo_copy.wait_recv()
    nobody = jnp.logical_and(r == 0, col == 0)
    for u in range(users):
        one_hot(jnp.where(nobody, -1.0, halo[u].astype(F32)), u, 0, HALO)

    joined = (joined_even, joined_odd)

    def gather(u, slot, turn):
        rows = dot(hot[u], projected[slot])
        for half in range(2):
            joined[turn][half] = rows[:, half * STRETCH : (half + 1) * STRETCH]

    def convolve(turn, half, weights, columns):
        total = None
        for k in range(weights.shape[0]):
            begin = HALO - weights.shape[0] + 1 + k
            term = joined[turn][half, begin : begin + events, :] * weights[k : k + 1, columns]
            total = term if total is None else total + term
        return total

    def make_maps(u):
        into = convolve(u, 0, taps, slice(inner, inner + STRETCH)).astype(BF16)
        outs = convolve(u, 1, taps, slice(inner + STRETCH, inner + CHUNK))
        outward[u] = outs.astype(BF16)
        for c in range(stretches):
            rows = slice(c * STRETCH, (c + 1) * STRETCH)
            in_rows[u, :, rows] = jnp.transpose(into[rows].astype(F32))

    x_copies = {}
    order = [(d, u) for u in range(users) for d in shares_order[:3]]
    order += [(0, u) for u in range(users)]

    def state_step(i, prefetch=True):
        d, u = order[i]
        if prefetch and i + 1 < len(order):
            gather(order[i + 1][1], order[i + 1][0], (i + 1) % 2)
        for half in range(2):
            columns = share(d, half * STRETCH, STRETCH)
            values = silu_of_half(convolve(i % 2, half, half_taps, columns)).astype(BF16)
            signal[u, :, columns] = values
            scaled = (in_rows[u] * tails[u, 2 * row_peer(d) + half]).astype(BF16)
            state = dot(scaled, values).astype(BF16)
            cols = slice(half * STRETCH, (half + 1) * STRETCH)
            if d:
                states[u, d, :, cols] = state
            else:
                row_states[u, r, :, cols] = state
        if d:
            x_copies[u, d] = send(
                states.at[u, d],
                row_states.at[u, r],
                x_send.at[u, d],
                x_recv.at[u, d],
                to_row(d),
            )

    gather(0, ROWS, 0)
    gather(1, ROWS, 1)
    make_maps(0)
    gather(0, 2, 0)
    make_maps(1)
    for i in range(3):
        state_step(i)

    for copy in xl_copies:
        copy.wait_recv()
    block_log = row_logs[0]
    for i in range(1, ROWS):
        block_log = block_log + row_logs[i]
    z_log_out[...] = block_log
    z_logs[z] = block_log
    pl.semaphore_wait(near.at[2], 2)
    pl.semaphore_wait(near.at[3], 2)
    zl_copies = [
        send(z_log_out, z_logs.at[z], zl_send.at[d], zl_recv.at[d], to_z(d)) for d in range(1, ZS)
    ]

    for i in range(3, len(order)):
        state_step(i)

    loads[13].wait()

    def gate_phase(begin, end):
        @pl.loop(begin, end)
        def _(j):
            columns = pl.ds(pl.multiple_of(j * WIDE, WIDE), WIDE)
            opened = dot(table[...], w_gate[:, columns]).astype(BF16)
            opened = silu_of_half(0.5 * opened.astype(F32)).astype(BF16)
            for u in range(users):
                gate[u, :, columns] = dot(hot[u, HALO:, :], opened).astype(BF16)

    def local_phase(u, begin, end):
        @pl.loop(begin, end)
        def _(c):
            rows = pl.ds(pl.multiple_of(c * STRETCH, STRETCH), STRETCH)
            column = columns_out[u, rows, :]
            log_t = log_rows[u, c]
            step_t = step_rows[u, c]
            last = log_t[:, STRETCH - 1 :]
            tail_t = jnp.exp(log_t - last) * step_t
            stay = jnp.exp(-last)
            outs = outward[u, rows, :]
            in_t = in_rows[u, :, rows]
            scores = dot(outs, in_t.astype(BF16))
            for h in range(heads):
                cols = slice(h * STRETCH, (h + 1) * STRETCH)
                gap = jnp.where(causal, log_t[h : h + 1, :] - column[:, h : h + 1], -1e30)
                weights = (scores * jnp.exp(gap) * step_t[h : h + 1, :]).astype(BF16)
                values = signal[u, rows, cols]
                entering = jnp.where(c == 0, 0.0, running[:, cols])
                fade = column[:, 3 * heads + h : 3 * heads + h + 1]
                mix[u, rows, cols] = (
                    dot(weights, values) + dot(outs, entering.astype(BF16)) * fade
                ).astype(BF16)
                scaled = (in_t * tail_t[h : h + 1, :]).astype(BF16)
                running[:, cols] = stay[h : h + 1, :] * entering + dot(scaled, values)

    gate_phase(0, 1)

    for u in range(users):
        for d in range(1, ROWS):
            x_copies[u, d].wait_recv()
        total = row_states[u, 0].astype(F32)
        for i in range(1, ROWS):
            for k in range(ZS):
                row_before[i - 1, k, u] = total[k * part : (k + 1) * part]
            total = jnp.exp(-row_logs[i, u]) * total + row_states[u, i].astype(F32)
        block = total.astype(BF16)
        for k in range(ZS):
            z_out[k, u] = block[k * part : (k + 1) * part]
    z_states[z] = z_out[z]
    z_copies = [
        send(z_out.at[z_peer(d)], z_states.at[z], z_send.at[d], z_recv.at[d], to_z(d))
        for d in (4, 3, 5, 2, 6, 1, 7)
    ]

    gate_phase(1, inner // WIDE)
    local_phase(0, 0, 3)

    for copy in zl_copies:
        copy.wait_recv()
    y_log = z_logs[0]
    for i in range(1, ZS):
        y_log = y_log + z_logs[i]
    y_log_out[...] = y_log
    y_logs[y] = y_log
    yl_copies = [
        send(y_log_out, y_logs.at[y], yl_send.at[d], yl_recv.at[d], to_y(d)) for d in range(1, YS)
    ]

    for copy in z_copies:
        copy.wait_recv()
    total = z_states[0].astype(F32)
    for i in range(1, ZS):
        z_before[i - 1] = total
        total = jnp.exp(-z_logs[i]) * total + z_states[i].astype(F32)
    y_out[...] = total.astype(BF16)
    y_copies = [
        send(y_out, y_states.at[y], y_send.at[d], y_recv.at[d], to_y(d)) for d in (2, 1, 3)
    ]

    local_phase(0, 3, stretches)
    local_phase(1, 0, 2)

    for copy in yl_copies:
        copy.wait_recv()
    for copy in y_copies:
        copy.wait_recv()
    entering = jnp.zeros(y_out.shape, F32)
    for i in range(YS - 1):
        entering = jnp.where(
            i < y, jnp.exp(-y_logs[i]) * entering + y_states[i].astype(F32), entering
        )
    gone = None
    for k in range(ZS):
        value = entering
        if k:
            gone = z_logs[k - 1] if gone is None else gone + z_logs[k - 1]
            value = jnp.exp(-gone) * entering + z_before[k - 1]
        c_out[k] = value.astype(BF16)
    c_states[z] = c_out[z]
    c_copies = {
        d: send(c_out.at[z_peer(d)], c_states.at[z], c_send.at[d], c_recv.at[d], to_z(d))
        for d in (4, 3, 5, 2, 6, 1, 7)
    }

    gone = [None, row_logs[0]]
    for i in range(2, ROWS):
        gone.append(gone[-1] + row_logs[i - 1])
    kept = [None] + [jnp.exp(-gone[i]) for i in range(1, ROWS)]
    b_copies = []

    def forward(d):
        k = z_peer(ZS - d)
        value = c_states[k].astype(F32)
        back_out[0, k] = c_states[k]
        for i in range(1, ROWS):
            back_out[i, k] = (kept[i] * value + row_before[i - 1, k]).astype(BF16)
        carry[r, k] = back_out[r, k]
        for x in (2, 1, 3):
            b_copies.append(
                send(
                    back_out.at[row_peer(x), k],
                    carry.at[r, k],
                    b_send.at[x, d],
                    b_recv.at[x, d],
                    to_row(x),
                )
            )

    forward(0)
    local_phase(1, 2, 3)
    for begin, ends in ((3, (1, 7)), (4, (2, 6)), (4, (3, 5, 4))):
        for d in ends:
            c_copies[d].wait_recv()
            forward(d)
        if begin < stretches:
            local_phase(1, begin, begin + 1)

    for load in loads[14:]:
        load.wait()

    for u in range(users):
        held = carry[r, :, u].reshape(STRETCH, CHUNK)
        for c in range(stretches):
            rows = slice(c * STRETCH, (c + 1) * STRETCH)
            carried = dot(outward[u, rows, :], held)
            both = None
            for half in range(2):
                cols = share(0, half * STRETCH, STRETCH)
                place = 2 * heads + half
                value = (
                    columns_out[u, rows, place : place + 1]
                    * carried[:, half * STRETCH : (half + 1) * STRETCH]
                    + mix[u, rows, cols].astype(F32)
                ) * gate[u, rows, cols].astype(F32)
                gated[rows, half * STRETCH : (half + 1) * STRETCH] = (
                    value * gain[:, cols]
                ).astype(BF16)
                both = value * value if both is None else both + value * value
            squares[u, rows, :] = both
        for j in range(w_out.shape[1] // CHUNK):
            columns = slice(j * CHUNK, (j + 1) * CHUNK)
            total_out[u, :, columns] = dot(gated[...], w_out[:, columns])
    for copy in b_copies:
        copy.wait_recv()
    for copy in sent:
        copy.wait_send()


def final_kernel(
    carry,
    mix,
    gate,
    outward,
    columns_in,
    totals,
    partial,
    gain,
    w_out,
    result,
    gated,
    squares,
    done,
    sems,
):
    users, events, inner = mix.shape
    heads = inner // STRETCH
    width = w_out.shape[1]
    block = 2 * STRETCH
    copies = []
    scale = {}

    def owner(d, begin=0, size=CHUNK):
        place = lax.rem(lax.axis_index("row") + d, ROWS) * CHUNK + begin
        return pl.ds(pl.multiple_of(place, STRETCH), size)

    def open_gate(u, c, d):
        rows = slice(c * block, (c + 1) * block)
        held = carry[lax.rem(lax.axis_index("row") + d, ROWS), :, u].reshape(STRETCH, CHUNK)
        carried = dot(outward[u, rows, :], held)
        added = None
        for half in range(2):
            cols = owner(d, half * STRETCH, STRETCH)
            place = 2 * heads + 2 * d + half
            value = (
                columns_in[u, rows, place : place + 1]
                * carried[:, half * STRETCH : (half + 1) * STRETCH]
                + mix[u, rows, cols].astype(F32)
            ) * gate[u, rows, cols].astype(F32)
            begin = (d - 1) * CHUNK + half * STRETCH
            gated[u, rows, begin : begin + STRETCH] = (value * gain[:, cols]).astype(BF16)
            added = value * value if added is None else added + value * value
        before = partial if d == 1 else squares
        squares[u, rows, :] = before[u, rows, :] + added

    def scale_of(u):
        mean = jnp.sum(squares[u], axis=1, keepdims=True) * (1.0 / inner)
        scale[u] = lax.rsqrt(mean + 1.0) * columns_in[u, :, heads : heads + 1]

    def project(u, j):
        columns = slice(j * CHUNK, (j + 1) * CHUNK)
        values = totals[u, :, columns]
        for d in range(1, ROWS):
            values = values + dot(
                gated[u, :, (d - 1) * CHUNK : d * CHUNK], w_out[owner(d), columns]
            )
        done[u, :, columns] = (values * scale[u]).astype(BF16)

    def store(u, j):
        columns = slice(j * CHUNK, (j + 1) * CHUNK)
        copy = pltpu.make_async_copy(
            done.at[u, :, columns], result.at[u, 0, :, columns], sems.at[u, j]
        )
        copy.start()
        copies.append(copy)

    steps = [(c, d) for c in range(events // block) for d in range(1, ROWS)]
    for c, d in steps:
        open_gate(0, c, d)
    for u in range(users):
        scale_of(u)
        left = list(steps)
        for j in range(width // CHUNK):
            project(u, j)
            for _ in range(2):
                if u + 1 < users and left:
                    open_gate(u + 1, *left.pop(0))
            store(u, j)
    for copy in copies:
        copy.wait()


def per_device(
    item_ids,
    pad_masks,
    lengths,
    item_table,
    w_gate,
    w_in,
    w_dt,
    conv_taps,
    dt_bias,
    decay_rates,
    norm_gain,
    w_out,
):
    users, _, events = item_ids.shape
    items, width = item_table.shape
    inner = w_gate.shape[1]
    full = w_in.shape[1]
    heads = decay_rates.shape[0]
    stretches = events // STRETCH
    pair = 2 * STRETCH
    part = STRETCH // ZS
    vmem = pl.BlockSpec(memory_space=pltpu.VMEM)
    hbm = pl.BlockSpec(memory_space=pltpu.HBM)
    dma = pltpu.SemaphoreType.DMA
    carry, mix, gate, outward, columns, totals, squares = pl.pallas_call(
        main_kernel,
        name="main",
        out_shape=(
            jax.ShapeDtypeStruct((ROWS, ZS, users, part, pair), BF16),
            jax.ShapeDtypeStruct((users, events, inner), BF16),
            jax.ShapeDtypeStruct((users, events, inner), BF16),
            jax.ShapeDtypeStruct((users, events, STRETCH), BF16),
            jax.ShapeDtypeStruct((users, events, STRETCH), F32),
            jax.ShapeDtypeStruct((users, events, w_out.shape[1]), F32),
            jax.ShapeDtypeStruct((users, events, STRETCH), F32),
        ),
        in_specs=[hbm] * 12,
        out_specs=(vmem,) * 7,
        scratch_shapes=[
            pltpu.SMEM(lengths.shape, lengths.dtype),
            pltpu.VMEM(item_ids.shape, item_ids.dtype),
            pltpu.VMEM(pad_masks.shape, pad_masks.dtype),
            pltpu.VMEM((heads, width), BF16),
            pltpu.VMEM(conv_taps.shape, F32),
            pltpu.VMEM((1, heads), F32),
            pltpu.VMEM((1, heads), F32),
            pltpu.VMEM((items, width), BF16),
            pltpu.VMEM((width, full), BF16),
            pltpu.VMEM((width, inner), BF16),
            pltpu.VMEM((CHUNK, w_out.shape[1]), BF16),
            pltpu.VMEM((1, inner), F32),
            pltpu.VMEM(conv_taps.shape, F32),
            pltpu.VMEM((users, stretches, 2 * heads, STRETCH), F32),
            pltpu.VMEM((events, CHUNK), BF16),
            pltpu.VMEM((STRETCH, width), BF16),
            pltpu.VMEM((items, 2 * STRETCH), BF16),
            pltpu.VMEM((users, 1, STRETCH), jnp.int32),
            pltpu.VMEM((users, HALO + events, items), BF16),
            pltpu.VMEM((ROWS + 1, items, CHUNK), BF16),
            pltpu.VMEM((2, HALO + events, STRETCH), F32),
            pltpu.VMEM((2, HALO + events, STRETCH), F32),
            pltpu.VMEM((users, events, inner), BF16),
            pltpu.VMEM((users, STRETCH, events), F32),
            pltpu.VMEM((users * stretches * heads, STRETCH), F32),
            pltpu.VMEM((users, stretches, heads, STRETCH), F32),
            pltpu.VMEM((users, stretches, heads, STRETCH), F32),
            pltpu.VMEM((users, heads, 1, events), F32),
            pltpu.VMEM((STRETCH, inner), F32),
            pltpu.VMEM((users, ROWS, STRETCH, pair), BF16),
            pltpu.VMEM((ROWS, users, 1, pair), F32),
            pltpu.VMEM((users, ROWS, STRETCH, pair), BF16),
            pltpu.VMEM((ROWS, users, 1, pair), F32),
            pltpu.VMEM((ROWS - 1, ZS, users, part, pair), F32),
            pltpu.VMEM((ZS, users, part, pair), BF16),
            pltpu.VMEM((ZS, users, part, pair), BF16),
            pltpu.VMEM((ZS - 1, users, part, pair), F32),
            pltpu.VMEM((users, 1, pair), F32),
            pltpu.VMEM((ZS, users, 1, pair), F32),
            pltpu.VMEM((users, part, pair), BF16),
            pltpu.VMEM((YS, users, part, pair), BF16),
            pltpu.VMEM((users, 1, pair), F32),
            pltpu.VMEM((YS, users, 1, pair), F32),
            pltpu.VMEM((ZS, users, part, pair), BF16),
            pltpu.VMEM((ZS, users, part, pair), BF16),
            pltpu.VMEM((ROWS, ZS, users, part, pair), BF16),
            dma((16,)),
            pltpu.SemaphoreType.REGULAR((4,)),
            dma,
            dma,
        ]
        + [dma((users, ROWS))] * 2
        + [dma((ROWS,))] * 2
        + [dma((ZS,))] * 4
        + [dma((YS,))] * 4
        + [dma((ZS,))] * 2
        + [dma((ROWS, ZS))] * 2,
        compiler_params=pltpu.CompilerParams(
            collective_id=0, has_side_effects=True, vmem_limit_bytes=36 << 20
        ),
    )(
        *(
            pltpu.with_memory_space_constraint(array, pltpu.HBM)
            for array in (
                lengths,
                item_ids,
                pad_masks,
                w_dt.T,
                conv_taps,
                dt_bias.reshape(1, heads),
                decay_rates.reshape(1, heads),
                item_table,
                w_in,
                w_gate,
                w_out,
                norm_gain.reshape(1, inner),
            )
        )
    )
    return pl.pallas_call(
        final_kernel,
        name="final",
        out_shape=jax.ShapeDtypeStruct((users, 1, events, w_out.shape[1]), BF16),
        in_specs=[vmem] * 9,
        out_specs=hbm,
        scratch_shapes=[
            pltpu.VMEM((users, events, 3 * CHUNK), BF16),
            pltpu.VMEM((users, events, STRETCH), F32),
            pltpu.VMEM((users, events, w_out.shape[1]), BF16),
            dma((users, w_out.shape[1] // CHUNK)),
        ],
        compiler_params=pltpu.CompilerParams(vmem_limit_bytes=16 << 20),
    )(carry, mix, gate, outward, columns, totals, squares, norm_gain.reshape(1, inner), w_out)


def solution(mesh):
    spans = P("batch", "col", "row")
    return jax.shard_map(
        per_device,
        mesh=mesh,
        in_specs=(spans, spans, P("batch")) + (P(),) * 9,
        out_specs=P("batch", "col", "row", None),
        check_vma=False,
    )
```
